32 devices in a mesh: row: 16 (over z, x, core), col: 2 (over y).
Axes of the slice: x: 2, y: 2, z: 4, core: 2. Of those that a mesh axis runs over, the one named last changes fastest.
Arguments:
- density: float32 [128, 16, 128, 128], P('row', 'col'), may hold values from -0.75 to 0.75
- columns: int32 [128, 16], P('row', 'col'), may hold values from -1 to 127, as said below
Outputs:
- purified: float32 [128, 16, 128, 128], P('row', 'col')
The draws below stay inside these ranges and needn't reach their ends.
Inputs may be any that keep to these rules, and one draw needn't show every extreme that they name: Block row i lists its occupied block columns in its first slots and -1 in the rest; it has 2 to 16 occupied slots, slot 0 holds column i, the listed columns of a row are distinct, and each listed column j satisfies (j - i) mod 128 <= 8 or (j - i) mod 128 >= 120.
All inputs are finite; a program needn't handle non-finite values.
Results may differ from the reference program's by a relative error of at most 0.0003.
Values sent between devices are 32-bit elements; how exact they have to be, the bound alone decides.
A program may use at most 128 MiB of HBM per device.

```python
import jax
import jax.numpy as jnp
from jax import lax

B = 128
S = 16
W = 8
NB = 128


def draw_columns(key, part):
    count_key, order_key = jax.random.split(jax.random.fold_in(key, 11))
    counts = jax.random.randint(count_key, (NB,), 2, S + 1).astype(jnp.int32)
    counts = counts.at[0].set(S)
    offsets = jnp.concatenate([jnp.arange(-W, 0), jnp.arange(1, W + 1)]).astype(jnp.int32)
    row_keys = jax.random.split(order_key, NB)
    shuffled = jax.vmap(lambda single: jax.random.permutation(single, offsets))(row_keys)
    chosen = jnp.concatenate([jnp.zeros((NB, 1), jnp.int32), shuffled[:, :S - 1]], axis=1)
    rows = jnp.arange(NB, dtype=jnp.int32)[:, None]
    listed = (rows + chosen) % NB
    slot_ids = jnp.arange(S, dtype=jnp.int32)[None, :]
    return jnp.where(slot_ids < counts[:, None], listed, -1).astype(jnp.int32)


def level_of(key, extent, cuts, smallest, top_value):
    level = 1.0
    for axis_at, parts in cuts:
        heights = jax.random.uniform(jax.random.fold_in(jax.random.fold_in(key, 6), axis_at), (parts,), jnp.float32, smallest / len(cuts), top_value / len(cuts))
        level = level * jnp.repeat(jnp.exp(heights), extent[axis_at] // parts).reshape((-1,) + (1,) * (len(extent) - 1 - axis_at))
    return level


def noise(stream_key, extent, scale, limit, shards=(), kind=jnp.bfloat16):
    loudness = level_of(stream_key, extent, shards, -0.22, 0.18) if shards else 1.0
    entries = jax.random.normal(stream_key, extent, jnp.float32) * scale * loudness
    return jnp.minimum(jnp.maximum(entries, -limit), limit).astype(kind)


def setup_inputs(seed: int = 0) -> dict:
    key_list = jax.random.split(jax.random.key(seed), 3)
    density = noise(key_list[0], (NB, S, B, B), 0.125, 0.75, ((0, 16), (1, 2)), jnp.float32)
    columns = draw_columns(jax.random.fold_in(key_list[2], 71), 0)
    return dict(density=density, columns=columns)


def pattern_product(left, right, columns):
    slots = columns.shape[1]

    def one_row(index):
        own = columns[index]
        safe = jnp.where(own >= 0, own, 0)
        candidate = columns[safe]
        matched = (candidate[None, :, :] == own[:, None, None]) & (own >= 0)[:, None, None] & (own >= 0)[None, :, None]
        weights = matched.astype(jnp.float32)
        chosen = jnp.einsum("sab,abxy->saxy", weights, right[safe], precision=lax.Precision.HIGHEST)
        return jnp.einsum("axk,sakc->sxc", left[index], chosen, precision=lax.Precision.HIGHEST)

    return lax.map(one_row, jnp.arange(columns.shape[0], dtype=jnp.int32))


def reference(density, columns):
    square = pattern_product(density, density, columns)
    cube = pattern_product(square, density, columns)
    return 3.0 * square - 2.0 * cube
```

```python
import functools

import jax
import jax.numpy as jnp
from jax import lax
from jax.experimental import pallas as pl
from jax.experimental.pallas import tpu as pltpu
from jax.sharding import PartitionSpec as P

W = 8
GROUP = 4
UNROLL = 2
CALLS = 2


def shifted(value, step):
    count = lax.axis_size("row")
    return lax.ppermute(value, "row", [(i, (i + step) % count) for i in range(count)])


def work_lists(ext_columns, own_start, panel_start, row_start, block_count, rows):
    slots = ext_columns.shape[1]
    own = lax.dynamic_slice_in_dim(ext_columns, W + own_start, rows)
    row_ids = jnp.arange(rows, dtype=jnp.int32)[:, None]
    offset = (own - (row_start + own_start + row_ids) + W) % block_count - W
    ext_row = jnp.where(own >= 0, W + own_start + row_ids + offset, 0)
    candidate = ext_columns[ext_row]
    matched = (
        (candidate[:, None] == own[:, :, None, None])
        & (own >= 0)[:, :, None, None]
        & (own >= 0)[:, None, :, None]
    )
    present = jnp.any(matched, axis=-1)
    slot_ids = jnp.arange(slots, dtype=jnp.int32)
    picked = jnp.sum(jnp.where(matched, slot_ids, 0), axis=-1)
    right = jnp.where(present, (ext_row - panel_start)[:, None, :] * slots + picked, 0)
    left = jnp.broadcast_to((row_ids * slots + slot_ids)[:, None, :], present.shape)
    targets = rows * slots
    present = present.reshape(targets, slots)
    rank = jnp.cumsum(present.astype(jnp.int32), axis=-1) - 1
    counts = jnp.sum(present.astype(jnp.int32), axis=-1)
    chosen = present[:, :, None] & (rank[:, :, None] == slot_ids)
    filled = slot_ids < counts[:, None]
    left_list = jnp.sum(jnp.where(chosen, left.reshape(targets, slots)[:, :, None], 0), axis=1)
    left_list = jnp.where(filled, left_list, targets)
    right_list = jnp.sum(jnp.where(chosen, right.reshape(targets, slots)[:, :, None], 0), axis=1)
    per_target = slots // GROUP
    chunks = (counts + GROUP - 1) // GROUP
    ends = jnp.cumsum(chunks)
    total = ends[-1]
    turns = jnp.arange(targets * per_target, dtype=jnp.int32)
    target = jnp.minimum(
        jnp.sum((ends[None, :] <= turns[:, None]).astype(jnp.int32), axis=1), targets - 1
    )
    place = jnp.clip(turns - (ends - chunks)[target], 0, per_target - 1)
    at = target * per_target + place
    live = (turns < total)[:, None]
    left_chunks = jnp.where(live, left_list.reshape(-1, GROUP)[at], targets)
    right_chunks = jnp.where(live, right_list.reshape(-1, GROUP)[at], 0)
    return total, target, left_chunks.reshape(-1), right_chunks.reshape(-1)


def split(value):
    high = value.astype(jnp.bfloat16)
    low = (value - high.astype(jnp.float32)).astype(jnp.bfloat16)
    return high, low


def kernel(sizes, slots, targets, meta, target_list, left_list, right_list, *refs):
    pieces = refs[: len(sizes)]
    out, stage, panel, left, square, sems = refs[len(sizes) :]
    order = out.shape[-1]
    starts = []
    at = 0
    for rows, width in sizes:
        starts.append(at)
        at += rows * width
    copies = [
        pltpu.make_async_copy(
            piece, stage.at[pl.ds(start, rows * width)], sems.at[number]
        )
        for number, (piece, start, (rows, width)) in enumerate(zip(pieces, starts, sizes))
    ]
    for copy in copies:
        copy.start()
    left[targets] = jnp.zeros((2 * order, order), jnp.bfloat16)

    def clear(block, carry):
        square[block] = jnp.zeros((order, order), jnp.float32)
        return carry

    lax.fori_loop(0, targets, clear, 0)
    for number, (copy, start, (rows, width)) in enumerate(zip(copies, starts, sizes)):
        copy.wait()
        first = meta[2 + number]

        def place(block, carry, start=start, width=width, first=first):
            high, low = split(stage[start + block])
            where = first + (block // width) * slots + block % width
            panel[where, :, :order] = high
            panel[where, :, order:] = low
            return carry

        lax.fori_loop(0, rows * width, place, 0)
    left_base = meta[1]

    def load_left(block, carry):
        left[block, :order] = panel[left_base + block, :, :order]
        left[block, order:] = panel[left_base + block, :, order:]
        return carry

    lax.fori_loop(0, targets, load_left, 0)
    rounds = (meta[0] + UNROLL - 1) // UNROLL

    def product(result, factor):
        def step(turn, carry):
            sums = []
            for inner in range(UNROLL):
                begin = (turn * UNROLL + inner) * GROUP
                lhs = jnp.concatenate([left[left_list[begin + g]] for g in range(GROUP)], axis=1)
                rhs = jnp.concatenate([panel[right_list[begin + g]] for g in range(GROUP)], axis=0)
                both = jnp.dot(lhs, rhs, preferred_element_type=jnp.float32)
                sums.append(
                    both[:order, :order]
                    + (both[:order, order:] + both[order:, :order])
                    + both[order:, order:]
                )
            for inner in range(UNROLL):
                target = target_list[turn * UNROLL + inner]
                result[target] += sums[inner] if factor == 1.0 else factor * sums[inner]
            return carry

        lax.fori_loop(0, rounds, step, 0)

    product(square, 1.0)

    def middle(block, carry):
        value = square[block]
        high, low = split(value)
        left[block, :order] = high
        left[block, order:] = low
        out[block] = 3.0 * value
        return carry

    lax.fori_loop(0, targets, middle, 0)
    product(out, -2.0)


def products(total, left_base, firsts, lists, pieces, panel_rows, slots, rows):
    order = pieces[0].shape[-1]
    sizes = tuple((piece.shape[0], piece.shape[1]) for piece in pieces)
    targets = rows * slots
    meta = jnp.stack([jnp.asarray(v, jnp.int32) for v in (total, left_base, *firsts)])
    blocks = sum(a * b for a, b in sizes)
    any_spec = pl.BlockSpec(memory_space=pl.ANY)
    smem_spec = pl.BlockSpec(memory_space=pltpu.SMEM)
    return pl.pallas_call(
        functools.partial(kernel, sizes, slots, targets),
        out_shape=jax.ShapeDtypeStruct((targets, order, order), jnp.float32),
        in_specs=[smem_spec] * 4 + [any_spec] * len(pieces),
        out_specs=pl.BlockSpec(memory_space=pltpu.VMEM),
        scratch_shapes=[
            pltpu.VMEM((blocks, order, order), jnp.float32),
            pltpu.VMEM((panel_rows * slots, order, 2 * order), jnp.bfloat16),
            pltpu.VMEM((targets + 1, 2 * order, order), jnp.bfloat16),
            pltpu.VMEM((targets, order, order), jnp.float32),
            pltpu.SemaphoreType.DMA((len(pieces),)),
        ],
        compiler_params=pltpu.CompilerParams(vmem_limit_bytes=62 * 1024 * 1024),
        cost_estimate=pl.CostEstimate(
            flops=8 * targets * 8 * order**3,
            bytes_accessed=blocks * order * order * 4,
            transcendentals=0,
        ),
    )(meta, *lists, *[piece.reshape(-1, order, order) for piece in pieces])


MESH = pl.DeviceIdType.MESH


def gather_kernel(
    dens, cols, panel, cols_out,
    own, peer, halo, halop, sib, sibp, stage,
    own_sem, ssem, rsem, csend, crecv, osem,
):
    rows, width = dens.shape[0], dens.shape[1]
    order = dens.shape[-1]
    slots = 2 * width
    half_rows = rows // 2
    count = lax.axis_size("row")
    r = lax.axis_index("row")
    y = lax.axis_index("col")
    core = r % 2
    lead = (core + y) % 2
    sibling = r + 1 - 2 * core
    side = 1 - 2 * y
    onward = (r + side + count) % count
    turn = 2 * core - 1
    near_row = (r + turn + count) % count
    next_row = (r + 2 * turn + count) % count
    from_row = (r - core - 1 + 3 * y + count) % count

    barrier = pltpu.get_barrier_semaphore()
    for row, column in (
        (r, 1 - y), (sibling, y), (sibling, 1 - y), (from_row, y), (from_row, 1 - y)
    ):
        pl.semaphore_signal(barrier, inc=1, device_id=(row, column), device_id_type=MESH)
    own_copy = pltpu.make_async_copy(dens, own, own_sem)
    own_copy.start()
    pl.semaphore_wait(barrier, 5)

    def remote(src, dst, send, recv, row, column):
        return pltpu.make_async_remote_copy(
            src_ref=src, dst_ref=dst, send_sem=send, recv_sem=recv,
            device_id=(row, column), device_id_type=MESH,
        )

    mine = (core + 1 - y) * 2 + y
    column_copies = [
        remote(cols, cols_out.at[place], csend.at[number], crecv.at[place], row, column)
        for number, (row, column, place) in enumerate((
            (r, 1 - y, (core + y) * 2 + y),
            (sibling, y, (core + 1 - y) * 2 + y),
            (sibling, 1 - y, (core + y) * 2 + y),
            (near_row, 1 - core, 2 * (1 - core) * 2 + y),
            (next_row, 1 - core, 2 * (1 - core) * 2 + y),
        ))
    ]

    def at(j):
        return (j + half_rows * (1 - y)) % rows

    def to_peer(j):
        q = (j + half_rows * y) % rows
        return remote(dens.at[q], peer.at[q], ssem.at[0, q], rsem.at[0, q], r, 1 - y)

    def own_onward(q):
        return remote(dens.at[q], halo.at[q], ssem.at[1, q], rsem.at[1, q], onward, y)

    def peer_onward(q):
        return remote(peer.at[q], halop.at[q], ssem.at[2, q], rsem.at[2, q], onward, y)

    def halo_across(q):
        return remote(halo.at[q], halo.at[q], ssem.at[1, q], rsem.at[1, q], sibling, y)

    def halop_across(q):
        return remote(halop.at[q], halop.at[q], ssem.at[2, q], rsem.at[2, q], sibling, y)

    def own_across(q):
        return remote(dens.at[q], sib.at[q], ssem.at[3, q], rsem.at[3, q], sibling, y)

    def peer_across(q):
        return remote(peer.at[q], sibp.at[q], ssem.at[4, q], rsem.at[4, q], sibling, y)

    def each(low, high, body):
        def step(j, carry):
            body(j)
            return carry

        lax.fori_loop(low, high, step, 0)

    own_at = jnp.where(y == 0, 8 + 4 * lead, 4 - 4 * lead) * half_rows // 4
    halo_at = jnp.where(y == 0, -4 * lead, 12 + 4 * lead) * half_rows // 4
    sib_at = jnp.where(y == 0, 16 - 12 * lead, -4 + 12 * lead) * half_rows // 4

    def out_copy(frame, half):
        where = pl.ds(frame * slots + half * width, width)
        return pltpu.make_async_copy(
            stage.at[where], panel.at[where], osem.at[frame * 2 + half]
        )

    def convert(source, q, first, half):
        frame = first + q

        def block(b, carry):
            high, low = split(source[q, b])
            where = frame * slots + half * width + b
            stage[where, :, :order] = high
            stage[where, :, order:] = low
            return carry

        lax.fori_loop(0, width, block, 0)
        out_copy(frame, half).start()

    @pl.when(lead == 0)
    def _():
        each(0, rows, lambda j: to_peer(j).start())

    @pl.when(lead == 1)
    def _():
        each(0, rows, lambda j: own_onward(at(j)).start())

    for copy in column_copies:
        copy.start()
    cols_out[mine] = cols[...]

    @pl.when(lead == 0)
    def _():
        each(0, rows, lambda j: own_across(at(j)).start())

    @pl.when(lead == 1)
    def _():
        each(half_rows, rows, lambda j: own_across(at(j)).start())

    own_copy.wait()
    each(0, rows, lambda q: convert(own, q, own_at, y))

    def landed(make, q):
        make(q).wait_recv()

    def peer_landed(q):
        remote(peer.at[q], peer.at[q], ssem.at[0, q], rsem.at[0, q], r, 1 - y).wait_recv()

    @pl.when(lead == 0)
    def _():
        def early(j):
            q = at(j)
            landed(halo_across, q)

            @pl.when(j < half_rows)
            def _():
                halo_across(q).start()

            convert(halo, q, halo_at, y)

            @pl.when(j >= half_rows)
            def _():
                landed(own_across, q)
                convert(sib, q, sib_at, y)
                landed(peer_across, q)
                convert(sibp, q, sib_at, 1 - y)

        each(0, rows, early)

        def late(j):
            q = at(j)
            peer_landed(q)
            peer_across(q).start()
            convert(peer, q, own_at, 1 - y)
            landed(halop_across, q)

            @pl.when(j < half_rows)
            def _():
                halop_across(q).start()

            convert(halop, q, halo_at, 1 - y)

        each(0, rows, late)

    @pl.when(lead == 1)
    def _():
        def early(j):
            q = at(j)
            peer_landed(q)
            peer_onward(q).start()

            @pl.when(j >= half_rows)
            def _():
                peer_across(q).start()

            @pl.when(j == rows - 2)
            def _():
                each(0, rows, lambda i: to_peer(i).start())

            convert(peer, q, own_at, 1 - y)
            landed(own_across, q)
            convert(sib, q, sib_at, y)

            @pl.when(j < half_rows)
            def _():
                landed(halo_across, q)
                convert(halo, q, halo_at, y)

        each(0, rows, early)

        def late(j):
            q = at(j)
            landed(peer_across, q)
            convert(sibp, q, sib_at, 1 - y)

            @pl.when(j < half_rows)
            def _():
                landed(halop_across, q)
                convert(halop, q, halo_at, 1 - y)

        each(0, rows, late)

    for number, place in enumerate((
        (core + 1 - y) * 2 + 1 - y,
        (2 - core - y) * 2 + y,
        (2 - core - y) * 2 + 1 - y,
        2 * y * 2 + y,
        2 * y * 2 + 1 - y,
    )):
        remote(cols, cols_out.at[place], csend.at[number], crecv.at[place], r, 1 - y).wait_recv()
    for copy in column_copies:
        copy.wait_send()
    each(0, rows, lambda j: to_peer(j).wait_send())

    @pl.when(lead == 0)
    def _():
        each(0, half_rows, lambda j: halo_across(at(j)).wait_send())
        each(0, half_rows, lambda j: halop_across(at(j)).wait_send())
        each(0, rows, lambda j: own_across(at(j)).wait_send())
        each(0, rows, lambda j: peer_across(at(j)).wait_send())

    @pl.when(lead == 1)
    def _():
        each(0, rows, lambda j: own_onward(at(j)).wait_send())
        each(0, rows, lambda j: peer_onward(at(j)).wait_send())
        each(half_rows, rows, lambda j: own_across(at(j)).wait_send())
        each(half_rows, rows, lambda j: peer_across(at(j)).wait_send())

    each(0, 2 * rows + half_rows, lambda f: out_copy(f, 0).wait())
    each(0, 2 * rows + half_rows, lambda f: out_copy(f, 1).wait())


def gather(density, columns):
    rows, width, order, _ = density.shape
    frames = 2 * rows + rows // 2
    blocks = frames * 2 * width
    lanes = 128
    padded = jnp.pad(columns, ((0, 0), (0, lanes - width)))
    any_spec = pl.BlockSpec(memory_space=pl.ANY)
    vmem_spec = pl.BlockSpec(memory_space=pltpu.VMEM)
    landing = pltpu.VMEM((rows, width, order, order), jnp.float32)
    return pl.pallas_call(
        gather_kernel,
        out_shape=(
            jax.ShapeDtypeStruct((blocks, order, 2 * order), jnp.bfloat16),
            jax.ShapeDtypeStruct((6, rows, lanes), jnp.int32),
        ),
        in_specs=[any_spec, vmem_spec],
        out_specs=(any_spec, vmem_spec),
        scratch_shapes=[landing] * 6
        + [
            pltpu.VMEM((blocks, order, 2 * order), jnp.bfloat16),
            pltpu.SemaphoreType.DMA,
            pltpu.SemaphoreType.DMA((5, rows)),
            pltpu.SemaphoreType.DMA((5, rows)),
            pltpu.SemaphoreType.DMA((5,)),
            pltpu.SemaphoreType.DMA((6,)),
            pltpu.SemaphoreType.DMA((2 * frames,)),
        ],
        compiler_params=pltpu.CompilerParams(
            vmem_limit_bytes=62 * 1024 * 1024, collective_id=0, has_side_effects=True
        ),
        cost_estimate=pl.CostEstimate(
            flops=10**9, bytes_accessed=blocks * order * order * 4, transcendentals=0
        ),
    )(density, padded)


def list_kernel(
    first, width, cols, panel, straight, crossed,
    pan, left, square, out, table, places, left_list, right_list, target_list, sem, out_sem,
):
    targets = square.shape[0]
    order = square.shape[-1]
    slots = 2 * width
    rows = targets // slots
    local_rows = cols.shape[1]
    frames = pan.shape[0] // slots
    span = table.shape[0] // (frames + 1)
    count = lax.axis_size("row")
    r = lax.axis_index("row")
    y = lax.axis_index("col")
    core = r % 2
    lead = (core + y) % 2
    block_count = count * local_rows
    shift = first + core * (local_rows // 2)
    base = ((r - core) * local_rows - W * (1 - y) + shift + block_count) % block_count
    load = pltpu.make_async_copy(
        panel.at[pl.ds(first * slots, frames * slots)], pan, sem
    )
    load.start()

    def column(frame, slot):
        row = frame + shift
        return cols[row // local_rows * 2 + slot // width, row % local_rows, slot % width]

    def offset(listed):
        away = listed - base
        away = jnp.where(away < 0, away + block_count, away)
        return away, (listed >= 0) & (away < frames)

    def clear_table(i, carry):
        for inner in range(frames + 1):
            table[inner * span + i] = 0
        return carry

    lax.fori_loop(0, span, clear_table, 0)
    unused = frames * span + span - 1

    def fill(frame, carry):
        for slot in range(slots):
            away, usable = offset(column(frame, slot))
            table[jnp.where(usable, frame * span + away, unused)] = frame * slots + slot + 1
        return carry

    lax.fori_loop(0, frames, fill, 0)

    def list_row(row, at):
        occupied = 0
        for slot in range(slots):
            listed = column(W + row, slot)
            away, _ = offset(listed)
            places[slot] = jnp.where(listed >= 0, away, frames)
            occupied += (listed >= 0).astype(jnp.int32)

        def list_target(slot, at):
            goal = places[slot]
            end = at
            for other in range(slots):
                found = table[places[other] * span + goal]
                left_list[end] = row * slots + other
                right_list[end] = found - 1
                end += (found > 0).astype(jnp.int32)
            for pad in range(GROUP - 1):
                left_list[end + pad] = targets
                right_list[end + pad] = 0
            chunks = (end - at + GROUP - 1) // GROUP
            for turn in range(slots // GROUP):
                target_list[at // GROUP + turn] = row * slots + slot
            return at + chunks * GROUP

        return lax.fori_loop(0, occupied, list_target, at)

    total = lax.fori_loop(0, rows, list_row, 0)
    for pad in range((UNROLL - 1) * GROUP):
        left_list[total + pad] = targets
        right_list[total + pad] = 0
    for pad in range(UNROLL - 1):
        target_list[total // GROUP + pad] = 0
    rounds = (total // GROUP + UNROLL - 1) // UNROLL

    left[targets] = jnp.zeros((2 * order, order), jnp.bfloat16)

    def clear(block, carry):
        square[block] = jnp.zeros((order, order), jnp.float32)
        return carry

    lax.fori_loop(0, targets, clear, 0)
    load.wait()

    def load_left(block, carry):
        left[block, :order] = pan[W * slots + block, :, :order]
        left[block, order:] = pan[W * slots + block, :, order:]
        return carry

    lax.fori_loop(0, targets, load_left, 0)

    def product(result, factor):
        def step(turn, carry):
            sums = []
            for inner in range(UNROLL):
                begin = (turn * UNROLL + inner) * GROUP
                lhs = jnp.concatenate([left[left_list[begin + g]] for g in range(GROUP)], axis=1)
                rhs = jnp.concatenate([pan[right_list[begin + g]] for g in range(GROUP)], axis=0)
                both = jnp.dot(lhs, rhs, preferred_element_type=jnp.float32)
                sums.append(
                    both[:order, :order]
                    + (both[:order, order:] + both[order:, :order])
                    + both[order:, order:]
                )
            for inner in range(UNROLL):
                target = target_list[turn * UNROLL + inner]
                result[target] += sums[inner] if factor == 1.0 else factor * sums[inner]
            return carry

        lax.fori_loop(0, rounds, step, 0)

    product(square, 1.0)

    def middle(block, carry):
        value = square[block]
        high, low = split(value)
        left[block, :order] = high
        left[block, order:] = low
        out[block] = 3.0 * value
        return carry

    lax.fori_loop(0, targets, middle, 0)
    product(out, -2.0)
    part = (1 + y + lead) % 2
    copies = []
    for row in range(rows):
        there = pl.ds(row * width, width)
        for number, (result, half) in enumerate(((straight, part), (crossed, 1 - part))):
            here = pl.ds(row * slots + half * width, width)
            copies.append(
                pltpu.make_async_copy(
                    out.at[here], result.at[there], out_sem.at[2 * row + number]
                )
            )
    for copy in copies:
        copy.start()
    for copy in copies:
        copy.wait()


def row_products(panel, columns, first, rows, width):
    order = panel.shape[1]
    slots = 2 * width
    targets = rows * slots
    frames = rows + 2 * W
    span = -(-(frames + 1) // 8) * 8
    any_spec = pl.BlockSpec(memory_space=pl.ANY)
    smem_spec = pl.BlockSpec(memory_space=pltpu.SMEM)
    result = jax.ShapeDtypeStruct((rows * width, order, order), jnp.float32)
    entries = targets * slots + UNROLL * GROUP
    return pl.pallas_call(
        functools.partial(list_kernel, first, width),
        out_shape=(result, result),
        in_specs=[smem_spec, any_spec],
        out_specs=(any_spec, any_spec),
        scratch_shapes=[
            pltpu.VMEM((frames * slots, order, 2 * order), jnp.bfloat16),
            pltpu.VMEM((targets + 1, 2 * order, order), jnp.bfloat16),
            pltpu.VMEM((targets, order, order), jnp.float32),
            pltpu.VMEM((targets, order, order), jnp.float32),
            pltpu.SMEM(((frames + 1) * span,), jnp.int32),
            pltpu.SMEM((slots,), jnp.int32),
            pltpu.SMEM((entries,), jnp.int32),
            pltpu.SMEM((entries,), jnp.int32),
            pltpu.SMEM((entries // GROUP + slots // GROUP,), jnp.int32),
            pltpu.SemaphoreType.DMA,
            pltpu.SemaphoreType.DMA((2 * rows,)),
        ],
        compiler_params=pltpu.CompilerParams(vmem_limit_bytes=62 * 1024 * 1024),
        cost_estimate=pl.CostEstimate(
            flops=8 * targets * 8 * order**3,
            bytes_accessed=frames * slots * order * order * 4,
            transcendentals=0,
        ),
    )(columns, panel)


def paired(density, columns):
    local_rows, width, order, _ = density.shape
    row_count = lax.axis_size("row")
    panel, listed = gather(density, columns)
    half = local_rows // 2
    portion = half // CALLS
    axes = ("row", "col")
    straight_pairs, crossed_pairs = [], []
    for r in range(row_count):
        for y in range(2):
            here = 2 * r + y
            sibling = r + 1 - 2 * (r % 2)
            if (r + y) % 2 == 0:
                straight_pairs.append((here, 2 * r + 1 - y))
                crossed_pairs.append((here, here))
            else:
                straight_pairs.append((here, 2 * sibling + y))
                crossed_pairs.append((here, 2 * sibling + 1 - y))
    straights, crosseds = [], []
    for call in range(CALLS):
        straight, crossed = row_products(panel, listed, call * portion, portion, width)
        straights.append(lax.ppermute(straight, axes, straight_pairs))
        crosseds.append(lax.ppermute(crossed, axes, crossed_pairs))
    shape = (local_rows, width, order, order)
    return jnp.where(
        lax.axis_index("col") == 0,
        jnp.concatenate(crosseds + straights).reshape(shape),
        jnp.concatenate(straights + crosseds).reshape(shape),
    )


def per_device(density, columns):
    local_rows, local_slots, order, _ = density.shape
    row_count = lax.axis_size("row")
    column_count = lax.axis_size("col")
    slots = local_slots * column_count
    if column_count == 2 and local_rows == W and row_count % 2 == 0 and row_count >= 6:
        return paired(density, columns)
    rows = local_rows // column_count
    block_count = local_rows * row_count
    row_start = lax.axis_index("row") * local_rows
    column = lax.axis_index("col")
    own_start = column * rows
    if column_count == 2:
        numbers = range(2 * row_count)
        around = 2 * row_count

        def from_row(step):
            same = [(i, (i - 2 * step) % around) for i in numbers]
            cross = [(i, ((i ^ 1) - 2 * step) % around) for i in numbers]
            mine = lax.ppermute(columns, ("row", "col"), same) if step else columns
            peer = lax.ppermute(columns, ("row", "col"), cross)
            return mine, peer

        parts = [from_row(step) for step in (-1, 0, 1)]
        density, parts = lax.optimization_barrier((density, parts))
        before, full_columns, after = [
            jnp.where(
                column == 0,
                jnp.concatenate([mine, peer], axis=1),
                jnp.concatenate([peer, mine], axis=1),
            )
            for mine, peer in parts
        ]
    else:
        full_columns = lax.all_gather(columns, "col", axis=1, tiled=True)
        before = shifted(full_columns, 1)
        after = shifted(full_columns, -1)
    ext_columns = jnp.concatenate([before[local_rows - W :], full_columns, after[:W]])
    trimmed = column_count == 2 and local_rows == W
    panel_start = own_start if trimmed else 0
    total, *lists = work_lists(
        ext_columns, own_start, panel_start, row_start, block_count, rows
    )
    if trimmed:
        ring = [(2 * i, 2 * ((i + 1) % row_count)) for i in range(row_count)]
        back = [(2 * ((i + 1) % row_count) + 1, 2 * i + 1) for i in range(row_count)]
        far_pairs = ring + back
        near_pairs = [(b, a) for a, b in far_pairs]
        peers = [(i, i ^ 1) for i in range(2 * row_count)]
        axes = ("row", "col")
        near_at = column * rows
        rest_at = (1 - column) * rows
        own_near = lax.dynamic_slice_in_dim(density, near_at, rows)
        own_rest = lax.dynamic_slice_in_dim(density, rest_at, rows)
        other_near = lax.ppermute(own_rest, axes, peers)
        far_own = lax.ppermute(density, axes, far_pairs)
        near_own = lax.ppermute(own_near, axes, near_pairs)
        second, other_near = lax.optimization_barrier((own_near, other_near))
        other_rest = lax.ppermute(second, axes, peers)
        near_other = lax.ppermute(other_near, axes, near_pairs)
        far_other_near = lax.ppermute(other_near, axes, far_pairs)
        far_other_rest = lax.ppermute(other_rest, axes, far_pairs)
        pieces = [
            density,
            far_own,
            near_own,
            other_near,
            other_rest,
            near_other,
            far_other_near,
            far_other_rest,
        ]
        own_row = W - own_start
        far_row = jnp.where(column == 0, 0, rows + local_rows)
        near_row = jnp.where(column == 0, W + local_rows, 0)
        here = column * local_slots
        there = (1 - column) * local_slots
        firsts = [
            own_row * slots + here,
            far_row * slots + here,
            near_row * slots + here,
            (own_row + near_at) * slots + there,
            (own_row + rest_at) * slots + there,
            near_row * slots + there,
            (far_row + near_at) * slots + there,
            (far_row + rest_at) * slots + there,
        ]
        panel_rows = 2 * W + rows
    else:
        full_rows = lax.all_gather(density, "col", axis=1, tiled=True)
        pieces = [
            shifted(full_rows[local_rows - W :], 1),
            full_rows,
            shifted(full_rows[:W], -1),
        ]
        firsts = [0, W * slots, (W + local_rows) * slots]
        panel_rows = 2 * W + local_rows
    left_base = (W + own_start - panel_start) * slots
    result = products(total, left_base, firsts, lists, pieces, panel_rows, slots, rows)
    result = result.reshape(rows, slots, order, order)
    if column_count != 2:
        return lax.all_to_all(result, "col", split_axis=1, concat_axis=0, tiled=True)
    kept = lax.dynamic_slice_in_dim(result, column * local_slots, local_slots, axis=1)
    sent = lax.dynamic_slice_in_dim(result, (1 - column) * local_slots, local_slots, axis=1)
    arrived = lax.ppermute(sent, "col", [(0, 1), (1, 0)])
    return jnp.where(
        column == 0,
        jnp.concatenate([kept, arrived]),
        jnp.concatenate([arrived, kept]),
    )


def solution(mesh):
    in_specs = (P("row", "col", None, None), P("row", "col"))
    out_specs = P("row", "col", None, None)
    return jax.shard_map(
        per_device, mesh=mesh, in_specs=in_specs, out_specs=out_specs, check_vma=False
    )
```

```python
import functools

import jax
import jax.numpy as jnp
from jax import lax
from jax.experimental import pallas as pl
from jax.experimental.pallas import tpu as pltpu
from jax.sharding import PartitionSpec as P

W = 8
GROUP = 4
UNROLL = 2
SPAN = 4


def shifted(value, step):
    count = lax.axis_size("row")
    return lax.ppermute(value, "row", [(i, (i + step) % count) for i in range(count)])


def work_lists(ext_columns, own_start, panel_start, row_start, block_count, rows):
    slots = ext_columns.shape[1]
    own = lax.dynamic_slice_in_dim(ext_columns, W + own_start, rows)
    row_ids = jnp.arange(rows, dtype=jnp.int32)[:, None]
    offset = (own - (row_start + own_start + row_ids) + W) % block_count - W
    ext_row = jnp.where(own >= 0, W + own_start + row_ids + offset, 0)
    candidate = ext_columns[ext_row]
    matched = (
        (candidate[:, None] == own[:, :, None, None])
        & (own >= 0)[:, :, None, None]
        & (own >= 0)[:, None, :, None]
    )
    present = jnp.any(matched, axis=-1)
    slot_ids = jnp.arange(slots, dtype=jnp.int32)
    picked = jnp.sum(jnp.where(matched, slot_ids, 0), axis=-1)
    right = jnp.where(present, (ext_row - panel_start)[:, None, :] * slots + picked, 0)
    left = jnp.broadcast_to((row_ids * slots + slot_ids)[:, None, :], present.shape)
    targets = rows * slots
    present = present.reshape(targets, slots)
    rank = jnp.cumsum(present.astype(jnp.int32), axis=-1) - 1
    counts = jnp.sum(present.astype(jnp.int32), axis=-1)
    chosen = present[:, :, None] & (rank[:, :, None] == slot_ids)
    filled = slot_ids < counts[:, None]
    left_list = jnp.sum(jnp.where(chosen, left.reshape(targets, slots)[:, :, None], 0), axis=1)
    left_list = jnp.where(filled, left_list, targets)
    right_list = jnp.sum(jnp.where(chosen, right.reshape(targets, slots)[:, :, None], 0), axis=1)
    per_target = slots // GROUP
    chunks = (counts + GROUP - 1) // GROUP
    ends = jnp.cumsum(chunks)
    total = ends[-1]
    turns = jnp.arange(targets * per_target, dtype=jnp.int32)
    target = jnp.minimum(
        jnp.sum((ends[None, :] <= turns[:, None]).astype(jnp.int32), axis=1), targets - 1
    )
    place = jnp.clip(turns - (ends - chunks)[target], 0, per_target - 1)
    at = target * per_target + place
    live = (turns < total)[:, None]
    left_chunks = jnp.where(live, left_list.reshape(-1, GROUP)[at], targets)
    right_chunks = jnp.where(live, right_list.reshape(-1, GROUP)[at], 0)
    return total, target, left_chunks.reshape(-1), right_chunks.reshape(-1)


def split(value):
    high = value.astype(jnp.bfloat16)
    low = (value - high.astype(jnp.float32)).astype(jnp.bfloat16)
    return high, low


def kernel(sizes, slots, targets, meta, target_list, left_list, right_list, *refs):
    pieces = refs[: len(sizes)]
    out, stage, panel, left, square, sems = refs[len(sizes) :]
    order = out.shape[-1]
    starts = []
    at = 0
    for rows, width in sizes:
        starts.append(at)
        at += rows * width
    copies = [
        pltpu.make_async_copy(
            piece, stage.at[pl.ds(start, rows * width)], sems.at[number]
        )
        for number, (piece, start, (rows, width)) in enumerate(zip(pieces, starts, sizes))
    ]
    for copy in copies:
        copy.start()
    left[targets] = jnp.zeros((2 * order, order), jnp.bfloat16)

    def clear(block, carry):
        square[block] = jnp.zeros((order, order), jnp.float32)
        return carry

    lax.fori_loop(0, targets, clear, 0)
    for number, (copy, start, (rows, width)) in enumerate(zip(copies, starts, sizes)):
        copy.wait()
        first = meta[2 + number]

        def place(block, carry, start=start, width=width, first=first):
            high, low = split(stage[start + block])
            where = first + (block // width) * slots + block % width
            panel[where, :, :order] = high
            panel[where, :, order:] = low
            return carry

        lax.fori_loop(0, rows * width, place, 0)
    left_base = meta[1]

    def load_left(block, carry):
        left[block, :order] = panel[left_base + block, :, :order]
        left[block, order:] = panel[left_base + block, :, order:]
        return carry

    lax.fori_loop(0, targets, load_left, 0)
    rounds = (meta[0] + UNROLL - 1) // UNROLL

    def product(result, factor):
        def step(turn, carry):
            sums = []
            for inner in range(UNROLL):
                begin = (turn * UNROLL + inner) * GROUP
                lhs = jnp.concatenate([left[left_list[begin + g]] for g in range(GROUP)], axis=1)
                rhs = jnp.concatenate([panel[right_list[begin + g]] for g in range(GROUP)], axis=0)
                both = jnp.dot(lhs, rhs, preferred_element_type=jnp.float32)
                sums.append(
                    both[:order, :order]
                    + (both[:order, order:] + both[order:, :order])
                    + both[order:, order:]
                )
            for inner in range(UNROLL):
                target = target_list[turn * UNROLL + inner]
                result[target] += sums[inner] if factor == 1.0 else factor * sums[inner]
            return carry

        lax.fori_loop(0, rounds, step, 0)

    product(square, 1.0)

    def middle(block, carry):
        value = square[block]
        high, low = split(value)
        left[block, :order] = high
        left[block, order:] = low
        out[block] = 3.0 * value
        return carry

    lax.fori_loop(0, targets, middle, 0)
    product(out, -2.0)


def products(total, left_base, firsts, lists, pieces, panel_rows, slots, rows):
    order = pieces[0].shape[-1]
    sizes = tuple((piece.shape[0], piece.shape[1]) for piece in pieces)
    targets = rows * slots
    meta = jnp.stack([jnp.asarray(v, jnp.int32) for v in (total, left_base, *firsts)])
    blocks = sum(a * b for a, b in sizes)
    any_spec = pl.BlockSpec(memory_space=pl.ANY)
    smem_spec = pl.BlockSpec(memory_space=pltpu.SMEM)
    return pl.pallas_call(
        functools.partial(kernel, sizes, slots, targets),
        out_shape=jax.ShapeDtypeStruct((targets, order, order), jnp.float32),
        in_specs=[smem_spec] * 4 + [any_spec] * len(pieces),
        out_specs=pl.BlockSpec(memory_space=pltpu.VMEM),
        scratch_shapes=[
            pltpu.VMEM((blocks, order, order), jnp.float32),
            pltpu.VMEM((panel_rows * slots, order, 2 * order), jnp.bfloat16),
            pltpu.VMEM((targets + 1, 2 * order, order), jnp.bfloat16),
            pltpu.VMEM((targets, order, order), jnp.float32),
            pltpu.SemaphoreType.DMA((len(pieces),)),
        ],
        compiler_params=pltpu.CompilerParams(vmem_limit_bytes=62 * 1024 * 1024),
        cost_estimate=pl.CostEstimate(
            flops=8 * targets * 8 * order**3,
            bytes_accessed=blocks * order * order * 4,
            transcendentals=0,
        ),
    )(meta, *lists, *[piece.reshape(-1, order, order) for piece in pieces])


MESH = pl.DeviceIdType.MESH


def fused_kernel(
    dens, cols, result,
    own, peer, halo, halop, sib, sibp, stage, square, left, listed, lanes_ref, table, index,
    own_sem, ssem, rsem, csend, crecv, table_sem, osend, orecv,
):
    rows, width = dens.shape[0], dens.shape[1]
    order = dens.shape[-1]
    slots = 2 * width
    half_rows = rows // 2
    pairs = rows // 2
    targets = square.shape[0]
    nothing = stage.shape[0] - 1
    count = lax.axis_size("row")
    block_count = count * rows
    r = lax.axis_index("row")
    y = lax.axis_index("col")
    core = r % 2
    lead = (core + y) % 2
    sibling = r + 1 - 2 * core
    side = 1 - 2 * y
    onward = (r + side + count) % count
    turn = 2 * core - 1
    near_row = (r + turn + count) % count
    next_row = (r + 2 * turn + count) % count
    from_row = (r - core - 1 + 3 * y + count) % count

    barrier = pltpu.get_barrier_semaphore()
    for row, column in (
        (r, 1 - y), (sibling, y), (sibling, 1 - y), (from_row, y), (from_row, 1 - y)
    ):
        pl.semaphore_signal(barrier, inc=1, device_id=(row, column), device_id_type=MESH)
    own_copy = pltpu.make_async_copy(dens, own, own_sem)
    own_copy.start()
    pl.semaphore_wait(barrier, 5)

    def remote(src, dst, send, recv, row, column):
        return pltpu.make_async_remote_copy(
            src_ref=src, dst_ref=dst, send_sem=send, recv_sem=recv,
            device_id=(row, column), device_id_type=MESH,
        )

    mine = (core + 1 - y) * 2 + y
    column_copies = [
        remote(cols, listed.at[place], csend.at[number], crecv.at[place], row, column)
        for number, (row, column, place) in enumerate((
            (r, 1 - y, (core + y) * 2 + y),
            (sibling, y, (core + 1 - y) * 2 + y),
            (sibling, 1 - y, (core + y) * 2 + y),
            (near_row, 1 - core, 2 * (1 - core) * 2 + y),
            (next_row, 1 - core, 2 * (1 - core) * 2 + y),
        ))
    ]

    def order_of(j, plane):
        back = rows - 2 - 2 * (j // 2) + j % 2
        return back + (j - back) * plane

    def at(j):
        return order_of(j, y)

    def to_peer(j):
        q = order_of(j, 1 - y)
        return remote(dens.at[q], peer.at[q], ssem.at[0, q], rsem.at[0, q], r, 1 - y)

    def own_onward(q):
        return remote(dens.at[q], halo.at[q], ssem.at[1, q], rsem.at[1, q], onward, y)

    def peer_onward(q):
        return remote(peer.at[q], halop.at[q], ssem.at[2, q], rsem.at[2, q], onward, y)

    def halo_across(q):
        return remote(halo.at[q], halo.at[q], ssem.at[1, q], rsem.at[1, q], sibling, y)

    def halop_across(q):
        return remote(halop.at[q], halop.at[q], ssem.at[2, q], rsem.at[2, q], sibling, y)

    def own_across(q):
        return remote(dens.at[q], sib.at[q], ssem.at[3, q], rsem.at[3, q], sibling, y)

    def peer_across(q):
        return remote(peer.at[q], sibp.at[q], ssem.at[4, q], rsem.at[4, q], sibling, y)

    def each(low, high, body):
        def step(j, carry):
            body(j)
            return carry

        lax.fori_loop(low, high, step, 0)

    own_at = (8 + 4 * lead - y * (4 + 8 * lead)) * half_rows // 4
    halo_at = (-4 * lead + y * (12 + 8 * lead)) * half_rows // 4
    sib_at = (16 - 12 * lead + y * (-20 + 24 * lead)) * half_rows // 4

    def convert(source, q, first, half):
        def block(b, carry):
            high, low = split(source[q, b])
            where = (first + q) * slots + half * width + b
            stage[where, :, :order] = high
            stage[where, :, order:] = low
            return carry

        lax.fori_loop(0, width, block, 0)

    @pl.when(lead == 1)
    def _():
        each(0, rows, lambda j: own_onward(at(j)).start())
        each(0, rows, lambda j: to_peer(j).start())

    for copy in column_copies:
        copy.start()
    listed[mine] = cols[...]

    @pl.when(lead == 0)
    def _():
        each(0, rows, lambda j: own_across(at(j)).start())

    @pl.when(lead == 1)
    def _():
        each(half_rows, rows, lambda j: own_across(at(j)).start())

    stage[nothing] = jnp.zeros((order, 2 * order), jnp.bfloat16)

    def clear(block, carry):
        square[block] = jnp.zeros((order, order), jnp.float32)
        return carry

    lax.fori_loop(0, targets, clear, 0)

    for number, place in enumerate((
        (core + 1 - y) * 2 + 1 - y,
        (2 - core - y) * 2 + y,
        (2 - core - y) * 2 + 1 - y,
        2 * y * 2 + y,
        2 * y * 2 + 1 - y,
    )):
        remote(cols, listed.at[place], csend.at[number], crecv.at[place], r, 1 - y).wait_recv()
    for group in range(3):
        lanes_ref[group * rows : (group + 1) * rows] = listed[2 * group] + listed[2 * group + 1]
    reach = lanes_ref[...]
    grid = reach.shape
    shift = half_rows * core
    base = ((r - core) * rows - W * (1 - y) + block_count) % block_count
    lane = lax.broadcasted_iota(jnp.int32, grid, 1)
    line = lax.broadcasted_iota(jnp.int32, grid, 0)
    absolute = base + line
    absolute = jnp.where(absolute >= block_count, absolute - block_count, absolute)
    staged = (line >= shift) & (line < shift + nothing // slots)
    for row in range(half_rows):
        goal = jnp.broadcast_to(lanes_ref[pl.ds(W + row + shift, 1)], grid)
        goal = jnp.where((lane < slots) & (goal >= 0), goal, -2)
        right = jnp.full(grid, nothing, jnp.int32)
        from_left = jnp.full(grid, nothing, jnp.int32)
        for slot in range(slots):
            held = jnp.broadcast_to(reach[:, slot : slot + 1], grid)
            right = jnp.where((held == goal) & staged, (line - shift) * slots + slot, right)
            wanted = jnp.broadcast_to(goal[:, slot : slot + 1], grid)
            from_left = jnp.where(wanted == absolute, (W + row) * slots + slot, from_left)
        table[row, : grid[0]] = jnp.where(lane < 64, right, from_left)
        away = goal - base
        away = jnp.where(away < 0, away + block_count, away)
        usable = (goal >= 0) & (away >= shift) & (away < shift + nothing // slots)
        away = jnp.where(usable, away, shift)
        table[row, grid[0] : grid[0] + 8] = away[:8]
    fetch = pltpu.make_async_copy(table, index, table_sem)
    fetch.start()

    own_copy.wait()
    each(0, rows, lambda q: convert(own, q, own_at, y))
    fetch.wait()

    def quarters(both):
        return (
            both[:order, :order]
            + (both[:order, order:] + both[order:, :order])
            + both[order:, order:]
        )

    def pair(frame):
        low = jnp.maximum(frame - 2 * W, 0)
        high = jnp.minimum(frame + 2, half_rows)

        def one_row(row, carry):
            one = stage[index[row, frame + shift, 64]]
            two = stage[index[row, frame + 1 + shift, 64]]
            lhs = jnp.concatenate(
                [
                    jnp.concatenate([one[:, :order], two[:, :order]], axis=1),
                    jnp.concatenate([one[:, order:], two[:, order:]], axis=1),
                ],
                axis=0,
            )

            def some(step, carry):
                sums = []
                for inner in range(SPAN):
                    slot = step * SPAN + inner
                    rhs = jnp.concatenate(
                        [
                            stage[index[row, frame + shift, slot]],
                            stage[index[row, frame + 1 + shift, slot]],
                        ],
                        axis=0,
                    )
                    sums.append(quarters(jnp.dot(lhs, rhs, preferred_element_type=jnp.float32)))
                for inner in range(SPAN):
                    square[row * slots + step * SPAN + inner] += sums[inner]
                return carry

            return lax.fori_loop(0, slots // SPAN, some, carry)

        lax.fori_loop(low, high, one_row, 0)

    holder = r + (sibling - r) * lead
    first_row = half_rows * core

    def row_at(n):
        return half_rows - 1 - n + y * (2 * n + 1 - half_rows)

    def across_out(n):
        row = row_at(n)
        half = 1 - y
        return remote(
            square.at[pl.ds(row * slots + half * width, width)],
            result.at[first_row + row],
            osend.at[0, row], orecv.at[first_row + row], holder, 1 - y,
        )

    def kept_out(n):
        row = row_at(n)
        return pltpu.make_async_copy(
            square.at[pl.ds(row * slots + y * width, width)],
            result.at[first_row + row],
            osend.at[1, row],
        )

    def sibling_out(n):
        row = row_at(n)
        return remote(
            square.at[pl.ds(row * slots + y * width, width)],
            result.at[first_row + row],
            osend.at[1, row], orecv.at[first_row + row], sibling, y,
        )

    def send_row(n):
        across_out(n).start()

        @pl.when(lead == 0)
        def _():
            kept_out(n).start()

        @pl.when(lead == 1)
        def _():
            sibling_out(n).start()

    def cube(n):
        row = row_at(n)

        def middle(slot, carry):
            high, low = split(square[row * slots + slot])
            left[slot, :order] = high
            left[slot, order:] = low
            return carry

        lax.fori_loop(0, slots, middle, 0)

        @pl.when(n > 0)
        def _():
            send_row(n - 1)

        lines = [index[row, 3 * rows, slot] for slot in range(slots)]

        def one_target(slot, carry):
            both = None
            for group in range(slots // GROUP):
                members = range(group * GROUP, (group + 1) * GROUP)
                lhs = jnp.concatenate([left[m] for m in members], axis=1)
                rhs = jnp.concatenate(
                    [stage[index[row, lines[m], slot]] for m in members], axis=0
                )
                part = jnp.dot(lhs, rhs, preferred_element_type=jnp.float32)
                both = part if both is None else both + part
            where = row * slots + slot
            square[where] = 3.0 * square[where] - 2.0 * quarters(both)
            return carry

        lax.fori_loop(0, slots, one_target, 0)

    def landed(make, q):
        make(q).wait_recv()

    def peer_landed(q):
        remote(peer.at[q], peer.at[q], ssem.at[0, q], rsem.at[0, q], r, 1 - y).wait_recv()

    def lower(k):
        return at(2 * k)

    @pl.when(lead == 0)
    def _():
        def early(j):
            q = at(j)
            peer_landed(q)
            peer_across(q).start()

            @pl.when(j == rows - 3)
            def _():
                each(0, rows, lambda i: to_peer(i).start())

            landed(halo_across, q)

            @pl.when(j < half_rows)
            def _():
                halo_across(q).start()

            convert(peer, q, own_at, 1 - y)
            convert(halo, q, halo_at, y)

            @pl.when(j >= half_rows)
            def _():
                landed(own_across, q)
                convert(sib, q, sib_at, y)

        each(0, rows, early)

        def arrive(j):
            q = at(j)
            landed(halop_across, q)

            @pl.when(j < half_rows)
            def _():
                halop_across(q).start()

            convert(halop, q, halo_at, 1 - y)

        def sib_pair(k):
            for j in (2 * k, 2 * k + 1):
                landed(peer_across, at(j))
                convert(sibp, at(j), sib_at, 1 - y)
            pair(sib_at + lower(k))

        def late(k):
            arrive(2 * k)
            pair(own_at + lower(k))

            @pl.when(k == pairs - 1)
            def _():
                each(pairs // 2, pairs, sib_pair)
                each(0, half_rows // 2, cube)

            arrive(2 * k + 1)
            pair(halo_at + lower(k))

        each(0, pairs, late)
        each(half_rows // 2, half_rows, cube)

    @pl.when(lead == 1)
    def _():
        def early(k):
            for j in (2 * k, 2 * k + 1):
                q = at(j)
                landed(own_across, q)
                convert(sib, q, sib_at, y)
                landed(peer_across, q)
                convert(sibp, q, sib_at, 1 - y)

                @pl.when(j < half_rows)
                def _():
                    landed(halo_across, q)
                    convert(halo, q, halo_at, y)

            @pl.when(k >= pairs // 2)
            def _():
                pair(sib_at + lower(k - pairs // 2))

        each(0, pairs, early)

        def arrive(j):
            q = at(j)
            peer_landed(q)
            peer_onward(q).start()

            @pl.when(j >= half_rows)
            def _():
                peer_across(q).start()

            convert(peer, q, own_at, 1 - y)

        def late(k):
            arrive(2 * k)
            behind = k >= pairs // 2

            @pl.when(behind)
            def _():
                for j in (2 * k - half_rows, 2 * k - half_rows + 1):
                    landed(halop_across, at(j))
                    convert(halop, at(j), halo_at, 1 - y)

            pair(
                jnp.where(
                    behind, halo_at + lower(k - pairs // 2), sib_at + lower(k + pairs // 2)
                )
            )
            arrive(2 * k + 1)
            pair(own_at + lower(k))

        each(0, pairs, late)
        each(0, half_rows, cube)

    for copy in column_copies:
        copy.wait_send()
    each(0, rows, lambda j: to_peer(j).wait_send())

    @pl.when(lead == 0)
    def _():
        each(0, half_rows, lambda j: halo_across(at(j)).wait_send())
        each(0, half_rows, lambda j: halop_across(at(j)).wait_send())
        each(0, rows, lambda j: own_across(at(j)).wait_send())
        each(0, rows, lambda j: peer_across(at(j)).wait_send())

    @pl.when(lead == 1)
    def _():
        each(0, rows, lambda j: own_onward(at(j)).wait_send())
        each(0, rows, lambda j: peer_onward(at(j)).wait_send())
        each(half_rows, rows, lambda j: own_across(at(j)).wait_send())
        each(half_rows, rows, lambda j: peer_across(at(j)).wait_send())

    send_row(half_rows - 1)

    def out_landed(q):
        remote(
            square.at[pl.ds(0, width)], result.at[q], osend.at[0, 0], orecv.at[q], r, 1 - y
        ).wait_recv()

    each(0, half_rows, lambda n: across_out(n).wait_send())

    @pl.when(lead == 0)
    def _():
        each(0, half_rows, lambda n: kept_out(n).wait())
        each(0, half_rows, lambda n: out_landed(half_rows - first_row + n))

    @pl.when(lead == 1)
    def _():
        each(0, half_rows, lambda n: sibling_out(n).wait_send())
        each(0, rows, out_landed)


def paired(density, columns):
    rows, width, order, _ = density.shape
    slots = 2 * width
    frames = 2 * rows + rows // 2
    blocks = frames * slots
    targets = rows // 2 * slots
    lanes = 128
    padded = jnp.where(
        lax.axis_index("col") == 0,
        jnp.pad(columns, ((0, 0), (0, lanes - width))),
        jnp.pad(columns, ((0, 0), (width, lanes - slots))),
    )
    any_spec = pl.BlockSpec(memory_space=pl.ANY)
    vmem_spec = pl.BlockSpec(memory_space=pltpu.VMEM)
    landing = pltpu.VMEM((rows, width, order, order), jnp.float32)
    return pl.pallas_call(
        fused_kernel,
        out_shape=jax.ShapeDtypeStruct((rows, width, order, order), jnp.float32),
        in_specs=[any_spec, vmem_spec],
        out_specs=any_spec,
        scratch_shapes=[landing] * 6
        + [
            pltpu.VMEM((blocks + 1, order, 2 * order), jnp.bfloat16),
            pltpu.VMEM((targets, order, order), jnp.float32),
            pltpu.VMEM((slots, 2 * order, order), jnp.bfloat16),
            pltpu.VMEM((6, rows, lanes), jnp.int32),
            pltpu.VMEM((3 * rows, lanes), jnp.int32),
            pltpu.VMEM((rows // 2, 3 * rows + 8, lanes), jnp.int32),
            pltpu.SMEM((rows // 2, 3 * rows + 8, lanes), jnp.int32),
            pltpu.SemaphoreType.DMA,
            pltpu.SemaphoreType.DMA((5, rows)),
            pltpu.SemaphoreType.DMA((5, rows)),
            pltpu.SemaphoreType.DMA((5,)),
            pltpu.SemaphoreType.DMA((6,)),
            pltpu.SemaphoreType.DMA,
            pltpu.SemaphoreType.DMA((2, rows // 2)),
            pltpu.SemaphoreType.DMA((rows,)),
        ],
        compiler_params=pltpu.CompilerParams(
            vmem_limit_bytes=62 * 1024 * 1024, collective_id=0, has_side_effects=True
        ),
        cost_estimate=pl.CostEstimate(
            flops=16 * targets * slots * order**3,
            bytes_accessed=blocks * order * order * 4,
            transcendentals=0,
        ),
    )(density, padded)


def per_device(density, columns):
    local_rows, local_slots, order, _ = density.shape
    row_count = lax.axis_size("row")
    column_count = lax.axis_size("col")
    slots = local_slots * column_count
    if column_count == 2 and local_rows == W and row_count % 2 == 0 and row_count >= 6:
        return paired(density, columns)
    rows = local_rows // column_count
    block_count = local_rows * row_count
    row_start = lax.axis_index("row") * local_rows
    column = lax.axis_index("col")
    own_start = column * rows
    if column_count == 2:
        numbers = range(2 * row_count)
        around = 2 * row_count

        def from_row(step):
            same = [(i, (i - 2 * step) % around) for i in numbers]
            cross = [(i, ((i ^ 1) - 2 * step) % around) for i in numbers]
            mine = lax.ppermute(columns, ("row", "col"), same) if step else columns
            peer = lax.ppermute(columns, ("row", "col"), cross)
            return mine, peer

        parts = [from_row(step) for step in (-1, 0, 1)]
        density, parts = lax.optimization_barrier((density, parts))
        before, full_columns, after = [
            jnp.where(
                column == 0,
                jnp.concatenate([mine, peer], axis=1),
                jnp.concatenate([peer, mine], axis=1),
            )
            for mine, peer in parts
        ]
    else:
        full_columns = lax.all_gather(columns, "col", axis=1, tiled=True)
        before = shifted(full_columns, 1)
        after = shifted(full_columns, -1)
    ext_columns = jnp.concatenate([before[local_rows - W :], full_columns, after[:W]])
    trimmed = column_count == 2 and local_rows == W
    panel_start = own_start if trimmed else 0
    total, *lists = work_lists(
        ext_columns, own_start, panel_start, row_start, block_count, rows
    )
    if trimmed:
        ring = [(2 * i, 2 * ((i + 1) % row_count)) for i in range(row_count)]
        back = [(2 * ((i + 1) % row_count) + 1, 2 * i + 1) for i in range(row_count)]
        far_pairs = ring + back
        near_pairs = [(b, a) for a, b in far_pairs]
        peers = [(i, i ^ 1) for i in range(2 * row_count)]
        axes = ("row", "col")
        near_at = column * rows
        rest_at = (1 - column) * rows
        own_near = lax.dynamic_slice_in_dim(density, near_at, rows)
        own_rest = lax.dynamic_slice_in_dim(density, rest_at, rows)
        other_near = lax.ppermute(own_rest, axes, peers)
        far_own = lax.ppermute(density, axes, far_pairs)
        near_own = lax.ppermute(own_near, axes, near_pairs)
        second, other_near = lax.optimization_barrier((own_near, other_near))
        other_rest = lax.ppermute(second, axes, peers)
        near_other = lax.ppermute(other_near, axes, near_pairs)
        far_other_near = lax.ppermute(other_near, axes, far_pairs)
        far_other_rest = lax.ppermute(other_rest, axes, far_pairs)
        pieces = [
            density,
            far_own,
            near_own,
            other_near,
            other_rest,
            near_other,
            far_other_near,
            far_other_rest,
        ]
        own_row = W - own_start
        far_row = jnp.where(column == 0, 0, rows + local_rows)
        near_row = jnp.where(column == 0, W + local_rows, 0)
        here = column * local_slots
        there = (1 - column) * local_slots
        firsts = [
            own_row * slots + here,
            far_row * slots + here,
            near_row * slots + here,
            (own_row + near_at) * slots + there,
            (own_row + rest_at) * slots + there,
            near_row * slots + there,
            (far_row + near_at) * slots + there,
            (far_row + rest_at) * slots + there,
        ]
        panel_rows = 2 * W + rows
    else:
        full_rows = lax.all_gather(density, "col", axis=1, tiled=True)
        pieces = [
            shifted(full_rows[local_rows - W :], 1),
            full_rows,
            shifted(full_rows[:W], -1),
        ]
        firsts = [0, W * slots, (W + local_rows) * slots]
        panel_rows = 2 * W + local_rows
    left_base = (W + own_start - panel_start) * slots
    result = products(total, left_base, firsts, lists, pieces, panel_rows, slots, rows)
    result = result.reshape(rows, slots, order, order)
    if column_count != 2:
        return lax.all_to_all(result, "col", split_axis=1, concat_axis=0, tiled=True)
    kept = lax.dynamic_slice_in_dim(result, column * local_slots, local_slots, axis=1)
    sent = lax.dynamic_slice_in_dim(result, (1 - column) * local_slots, local_slots, axis=1)
    arrived = lax.ppermute(sent, "col", [(0, 1), (1, 0)])
    return jnp.where(
        column == 0,
        jnp.concatenate([kept, arrived]),
        jnp.concatenate([arrived, kept]),
    )


def solution(mesh):
    in_specs = (P("row", "col", None, None), P("row", "col"))
    out_specs = P("row", "col", None, None)
    return jax.shard_map(
        per_device, mesh=mesh, in_specs=in_specs, out_specs=out_specs, check_vma=False
    )
```

```python
import functools

import jax
import jax.numpy as jnp
from jax import lax
from jax.experimental import pallas as pl
from jax.experimental.pallas import tpu as pltpu
from jax.sharding import PartitionSpec as P

W = 8
GROUP = 4
UNROLL = 2
SPAN = 4
TRIGGER = 4


def shifted(value, step):
    count = lax.axis_size("row")
    return lax.ppermute(value, "row", [(i, (i + step) % count) for i in range(count)])


def work_lists(ext_columns, own_start, panel_start, row_start, block_count, rows):
    slots = ext_columns.shape[1]
    own = lax.dynamic_slice_in_dim(ext_columns, W + own_start, rows)
    row_ids = jnp.arange(rows, dtype=jnp.int32)[:, None]
    offset = (own - (row_start + own_start + row_ids) + W) % block_count - W
    ext_row = jnp.where(own >= 0, W + own_start + row_ids + offset, 0)
    candidate = ext_columns[ext_row]
    matched = (
        (candidate[:, None] == own[:, :, None, None])
        & (own >= 0)[:, :, None, None]
        & (own >= 0)[:, None, :, None]
    )
    present = jnp.any(matched, axis=-1)
    slot_ids = jnp.arange(slots, dtype=jnp.int32)
    picked = jnp.sum(jnp.where(matched, slot_ids, 0), axis=-1)
    right = jnp.where(present, (ext_row - panel_start)[:, None, :] * slots + picked, 0)
    left = jnp.broadcast_to((row_ids * slots + slot_ids)[:, None, :], present.shape)
    targets = rows * slots
    present = present.reshape(targets, slots)
    rank = jnp.cumsum(present.astype(jnp.int32), axis=-1) - 1
    counts = jnp.sum(present.astype(jnp.int32), axis=-1)
    chosen = present[:, :, None] & (rank[:, :, None] == slot_ids)
    filled = slot_ids < counts[:, None]
    left_list = jnp.sum(jnp.where(chosen, left.reshape(targets, slots)[:, :, None], 0), axis=1)
    left_list = jnp.where(filled, left_list, targets)
    right_list = jnp.sum(jnp.where(chosen, right.reshape(targets, slots)[:, :, None], 0), axis=1)
    per_target = slots // GROUP
    chunks = (counts + GROUP - 1) // GROUP
    ends = jnp.cumsum(chunks)
    total = ends[-1]
    turns = jnp.arange(targets * per_target, dtype=jnp.int32)
    target = jnp.minimum(
        jnp.sum((ends[None, :] <= turns[:, None]).astype(jnp.int32), axis=1), targets - 1
    )
    place = jnp.clip(turns - (ends - chunks)[target], 0, per_target - 1)
    at = target * per_target + place
    live = (turns < total)[:, None]
    left_chunks = jnp.where(live, left_list.reshape(-1, GROUP)[at], targets)
    right_chunks = jnp.where(live, right_list.reshape(-1, GROUP)[at], 0)
    return total, target, left_chunks.reshape(-1), right_chunks.reshape(-1)


def split(value):
    high = value.astype(jnp.bfloat16)
    low = (value - high.astype(jnp.float32)).astype(jnp.bfloat16)
    return high, low


def kernel(sizes, slots, targets, meta, target_list, left_list, right_list, *refs):
    pieces = refs[: len(sizes)]
    out, stage, panel, left, square, sems = refs[len(sizes) :]
    order = out.shape[-1]
    starts = []
    at = 0
    for rows, width in sizes:
        starts.append(at)
        at += rows * width
    copies = [
        pltpu.make_async_copy(
            piece, stage.at[pl.ds(start, rows * width)], sems.at[number]
        )
        for number, (piece, start, (rows, width)) in enumerate(zip(pieces, starts, sizes))
    ]
    for copy in copies:
        copy.start()
    left[targets] = jnp.zeros((2 * order, order), jnp.bfloat16)

    def clear(block, carry):
        square[block] = jnp.zeros((order, order), jnp.float32)
        return carry

    lax.fori_loop(0, targets, clear, 0)
    for number, (copy, start, (rows, width)) in enumerate(zip(copies, starts, sizes)):
        copy.wait()
        first = meta[2 + number]

        def place(block, carry, start=start, width=width, first=first):
            high, low = split(stage[start + block])
            where = first + (block // width) * slots + block % width
            panel[where, :, :order] = high
            panel[where, :, order:] = low
            return carry

        lax.fori_loop(0, rows * width, place, 0)
    left_base = meta[1]

    def load_left(block, carry):
        left[block, :order] = panel[left_base + block, :, :order]
        left[block, order:] = panel[left_base + block, :, order:]
        return carry

    lax.fori_loop(0, targets, load_left, 0)
    rounds = (meta[0] + UNROLL - 1) // UNROLL

    def product(result, factor):
        def step(turn, carry):
            sums = []
            for inner in range(UNROLL):
                begin = (turn * UNROLL + inner) * GROUP
                lhs = jnp.concatenate([left[left_list[begin + g]] for g in range(GROUP)], axis=1)
                rhs = jnp.concatenate([panel[right_list[begin + g]] for g in range(GROUP)], axis=0)
                both = jnp.dot(lhs, rhs, preferred_element_type=jnp.float32)
                sums.append(
                    both[:order, :order]
                    + (both[:order, order:] + both[order:, :order])
                    + both[order:, order:]
                )
            for inner in range(UNROLL):
                target = target_list[turn * UNROLL + inner]
                result[target] += sums[inner] if factor == 1.0 else factor * sums[inner]
            return carry

        lax.fori_loop(0, rounds, step, 0)

    product(square, 1.0)

    def middle(block, carry):
        value = square[block]
        high, low = split(value)
        left[block, :order] = high
        left[block, order:] = low
        out[block] = 3.0 * value
        return carry

    lax.fori_loop(0, targets, middle, 0)
    product(out, -2.0)


def products(total, left_base, firsts, lists, pieces, panel_rows, slots, rows):
    order = pieces[0].shape[-1]
    sizes = tuple((piece.shape[0], piece.shape[1]) for piece in pieces)
    targets = rows * slots
    meta = jnp.stack([jnp.asarray(v, jnp.int32) for v in (total, left_base, *firsts)])
    blocks = sum(a * b for a, b in sizes)
    any_spec = pl.BlockSpec(memory_space=pl.ANY)
    smem_spec = pl.BlockSpec(memory_space=pltpu.SMEM)
    return pl.pallas_call(
        functools.partial(kernel, sizes, slots, targets),
        out_shape=jax.ShapeDtypeStruct((targets, order, order), jnp.float32),
        in_specs=[smem_spec] * 4 + [any_spec] * len(pieces),
        out_specs=pl.BlockSpec(memory_space=pltpu.VMEM),
        scratch_shapes=[
            pltpu.VMEM((blocks, order, order), jnp.float32),
            pltpu.VMEM((panel_rows * slots, order, 2 * order), jnp.bfloat16),
            pltpu.VMEM((targets + 1, 2 * order, order), jnp.bfloat16),
            pltpu.VMEM((targets, order, order), jnp.float32),
            pltpu.SemaphoreType.DMA((len(pieces),)),
        ],
        compiler_params=pltpu.CompilerParams(vmem_limit_bytes=62 * 1024 * 1024),
        cost_estimate=pl.CostEstimate(
            flops=8 * targets * 8 * order**3,
            bytes_accessed=blocks * order * order * 4,
            transcendentals=0,
        ),
    )(meta, *lists, *[piece.reshape(-1, order, order) for piece in pieces])


MESH = pl.DeviceIdType.MESH


def fused_kernel(
    dens, cols, result,
    own, peer, halo, halop, sib, sibp, stage, square, left, listed, lanes_ref, table, index,
    own_sem, ssem, rsem, csend, crecv, table_sem, osend, orecv,
):
    rows, width = dens.shape[0], dens.shape[1]
    order = dens.shape[-1]
    slots = 2 * width
    half_rows = rows // 2
    pairs = rows // 2
    targets = square.shape[0]
    nothing = stage.shape[0] - 1
    count = lax.axis_size("row")
    block_count = count * rows
    r = lax.axis_index("row")
    y = lax.axis_index("col")
    core = r % 2
    lead = (core + y) % 2
    sibling = r + 1 - 2 * core
    side = 1 - 2 * y
    onward = (r + side + count) % count
    turn = 2 * core - 1
    near_row = (r + turn + count) % count
    next_row = (r + 2 * turn + count) % count
    from_row = (r - core - 1 + 3 * y + count) % count

    barrier = pltpu.get_barrier_semaphore()
    for row, column in (
        (r, 1 - y), (sibling, y), (sibling, 1 - y), (from_row, y), (from_row, 1 - y)
    ):
        pl.semaphore_signal(barrier, inc=1, device_id=(row, column), device_id_type=MESH)
    own_copy = pltpu.make_async_copy(dens, own, own_sem)
    own_copy.start()
    pl.semaphore_wait(barrier, 5)

    def remote(src, dst, send, recv, row, column):
        return pltpu.make_async_remote_copy(
            src_ref=src, dst_ref=dst, send_sem=send, recv_sem=recv,
            device_id=(row, column), device_id_type=MESH,
        )

    mine = (core + 1 - y) * 2 + y
    column_copies = [
        remote(cols, listed.at[place], csend.at[number], crecv.at[place], row, column)
        for number, (row, column, place) in enumerate((
            (r, 1 - y, (core + y) * 2 + y),
            (sibling, y, (core + 1 - y) * 2 + y),
            (sibling, 1 - y, (core + y) * 2 + y),
            (near_row, 1 - core, 2 * (1 - core) * 2 + y),
            (next_row, 1 - core, 2 * (1 - core) * 2 + y),
        ))
    ]

    def order_of(j, plane):
        back = rows - 2 - 2 * (j // 2) + j % 2
        return back + (j - back) * plane

    def at(j):
        return order_of(j, y)

    def left_order(j, plane):
        n = j // 2
        back = half_rows - 1 - n
        return back + (n - back) * plane + half_rows * (j % 2)

    def to_peer(j):
        early, late = order_of(j, 1 - y), left_order(j, 1 - y)
        q = early + (late - early) * lead
        return remote(dens.at[q], peer.at[q], ssem.at[0, q], rsem.at[0, q], r, 1 - y)

    def own_onward(q):
        return remote(dens.at[q], halo.at[q], ssem.at[1, q], rsem.at[1, q], onward, y)

    def peer_onward(q):
        return remote(peer.at[q], halop.at[q], ssem.at[2, q], rsem.at[2, q], onward, y)

    def halo_across(q):
        return remote(halo.at[q], halo.at[q], ssem.at[1, q], rsem.at[1, q], sibling, y)

    def halop_across(q):
        return remote(halop.at[q], halop.at[q], ssem.at[2, q], rsem.at[2, q], sibling, y)

    def own_across(q):
        return remote(dens.at[q], sib.at[q], ssem.at[3, q], rsem.at[3, q], sibling, y)

    def peer_across(q):
        return remote(peer.at[q], sibp.at[q], ssem.at[4, q], rsem.at[4, q], sibling, y)

    def each(low, high, body):
        def step(j, carry):
            body(j)
            return carry

        lax.fori_loop(low, high, step, 0)

    own_at = (8 + 4 * lead - y * (4 + 8 * lead)) * half_rows // 4
    halo_at = (-4 * lead + y * (12 + 8 * lead)) * half_rows // 4
    sib_at = (16 - 12 * lead + y * (-20 + 24 * lead)) * half_rows // 4

    def convert(source, q, first, half):
        def block(b, carry):
            high, low = split(source[q, b])
            where = (first + q) * slots + half * width + b
            stage[where, :, :order] = high
            stage[where, :, order:] = low
            return carry

        lax.fori_loop(0, width, block, 0)

    for copy in column_copies:
        copy.start()

    @pl.when(lead == 1)
    def _():
        each(0, rows - 2, lambda j: to_peer(j).start())
        each(0, rows, lambda j: own_onward(at(j)).start())

    listed[mine] = cols[...]

    @pl.when(lead == 0)
    def _():
        each(0, rows, lambda j: own_across(at(j)).start())

    @pl.when(lead == 1)
    def _():
        each(half_rows, rows, lambda j: own_across(at(j)).start())

    stage[nothing] = jnp.zeros((order, 2 * order), jnp.bfloat16)

    def clear(block, carry):
        square[block] = jnp.zeros((order, order), jnp.float32)
        return carry

    lax.fori_loop(0, targets, clear, 0)

    for number, place in enumerate((
        (core + 1 - y) * 2 + 1 - y,
        (2 - core - y) * 2 + y,
        (2 - core - y) * 2 + 1 - y,
        2 * y * 2 + y,
        2 * y * 2 + 1 - y,
    )):
        remote(cols, listed.at[place], csend.at[number], crecv.at[place], r, 1 - y).wait_recv()
    for group in range(3):
        lanes_ref[group * rows : (group + 1) * rows] = listed[2 * group] + listed[2 * group + 1]
    reach = lanes_ref[...]
    grid = reach.shape
    shift = half_rows * core
    base = ((r - core) * rows - W * (1 - y) + block_count) % block_count
    lane = lax.broadcasted_iota(jnp.int32, grid, 1)
    line = lax.broadcasted_iota(jnp.int32, grid, 0)
    absolute = base + line
    absolute = jnp.where(absolute >= block_count, absolute - block_count, absolute)
    staged = (line >= shift) & (line < shift + nothing // slots)
    for row in range(half_rows):
        goal = jnp.broadcast_to(lanes_ref[pl.ds(W + row + shift, 1)], grid)
        goal = jnp.where((lane < slots) & (goal >= 0), goal, -2)
        right = jnp.full(grid, nothing, jnp.int32)
        from_left = jnp.full(grid, nothing, jnp.int32)
        for slot in range(slots):
            held = jnp.broadcast_to(reach[:, slot : slot + 1], grid)
            right = jnp.where((held == goal) & staged, (line - shift) * slots + slot, right)
            wanted = jnp.broadcast_to(goal[:, slot : slot + 1], grid)
            from_left = jnp.where(wanted == absolute, (W + row) * slots + slot, from_left)
        table[row, : grid[0]] = jnp.where(lane < 64, right, from_left)
        away = goal - base
        away = jnp.where(away < 0, away + block_count, away)
        usable = (goal >= 0) & (away >= shift) & (away < shift + nothing // slots)
        away = jnp.where(usable, away, shift)
        table[row, grid[0] : grid[0] + 8] = away[:8]
    fetch = pltpu.make_async_copy(table, index, table_sem)
    fetch.start()

    own_copy.wait()
    each(0, rows, lambda q: convert(own, q, own_at, y))

    def quarters(both):
        return (
            both[:order, :order]
            + (both[:order, order:] + both[order:, :order])
            + both[order:, order:]
        )

    def reaching(frame):
        return jnp.maximum(frame - 2 * W, 0), jnp.minimum(frame + 2, half_rows)

    def near_pair(frame, first, last):
        low, high = reaching(frame)
        pair_rows(frame, frame + 1, jnp.maximum(low, first), jnp.minimum(high, last))

    def pair_rows(frame, other, low, high):
        def one_row(row, carry):
            one = stage[index[row, frame + shift, 64]]
            two = stage[index[row, other + shift, 64]]
            lhs = jnp.concatenate(
                [
                    jnp.concatenate([one[:, :order], two[:, :order]], axis=1),
                    jnp.concatenate([one[:, order:], two[:, order:]], axis=1),
                ],
                axis=0,
            )

            def some(step, carry):
                sums = []
                for inner in range(SPAN):
                    slot = step * SPAN + inner
                    rhs = jnp.concatenate(
                        [
                            stage[index[row, frame + shift, slot]],
                            stage[index[row, other + shift, slot]],
                        ],
                        axis=0,
                    )
                    sums.append(quarters(jnp.dot(lhs, rhs, preferred_element_type=jnp.float32)))
                for inner in range(SPAN):
                    square[row * slots + step * SPAN + inner] += sums[inner]
                return carry

            return lax.fori_loop(0, slots // SPAN, some, carry)

        lax.fori_loop(low, high, one_row, 0)

    holder = r + (sibling - r) * lead
    first_row = half_rows * core

    def row_at(n):
        return half_rows - 1 - n + y * (2 * n + 1 - half_rows)

    def across_out(n):
        row = row_at(n)
        half = 1 - y
        return remote(
            square.at[pl.ds(row * slots + half * width, width)],
            result.at[first_row + row],
            osend.at[0, row], orecv.at[first_row + row], holder, 1 - y,
        )

    def kept_out(n):
        row = row_at(n)
        return pltpu.make_async_copy(
            square.at[pl.ds(row * slots + y * width, width)],
            result.at[first_row + row],
            osend.at[1, row],
        )

    def sibling_out(n):
        row = row_at(n)
        return remote(
            square.at[pl.ds(row * slots + y * width, width)],
            result.at[first_row + row],
            osend.at[1, row], orecv.at[first_row + row], sibling, y,
        )

    def send_kept(n):
        @pl.when(lead == 0)
        def _():
            kept_out(n).start()

        @pl.when(lead == 1)
        def _():
            sibling_out(n).start()

    def cube(n):
        row = row_at(n)

        def middle(slot, carry):
            high, low = split(square[row * slots + slot])
            left[slot, :order] = high
            left[slot, order:] = low
            return carry

        lax.fori_loop(0, slots, middle, 0)

        @pl.when(n > 0)
        def _():
            send_kept(n - 1)

        lines = [index[row, 3 * rows, slot] for slot in range(slots)]

        def one_target(step, carry):
            slot = (step + width * (1 - y)) % slots
            both = None
            for group in range(slots // GROUP):
                members = range(group * GROUP, (group + 1) * GROUP)
                lhs = jnp.concatenate([left[m] for m in members], axis=1)
                rhs = jnp.concatenate(
                    [stage[index[row, lines[m], slot]] for m in members], axis=0
                )
                part = jnp.dot(lhs, rhs, preferred_element_type=jnp.float32)
                both = part if both is None else both + part
            where = row * slots + slot
            square[where] = 3.0 * square[where] - 2.0 * quarters(both)

            @pl.when(step == width)
            def _():
                across_out(n).start()

            return carry

        lax.fori_loop(0, slots, one_target, 0)

    def landed(make, q):
        make(q).wait_recv()

    def peer_landed(q):
        remote(peer.at[q], peer.at[q], ssem.at[0, q], rsem.at[0, q], r, 1 - y).wait_recv()

    def lower(k):
        return at(2 * k)

    def halo_arrive(j):
        q = at(j)
        landed(halop_across, q)

        @pl.when(j < half_rows * (1 - lead))
        def _():
            halop_across(q).start()

        convert(halop, q, halo_at, 1 - y)

    def left_arrive(j):
        q = left_order(j, y)

        @pl.when(lead == 0)
        def _():
            peer_landed(q)
            peer_across(q).start()
            convert(peer, q, own_at, 1 - y)

        @pl.when(lead == 1)
        def _():
            landed(peer_across, q)
            convert(sibp, q, sib_at, 1 - y)

    def onward_arrive(j):
        q = at(j)

        @pl.when(lead == 1)
        def _():
            peer_landed(q)
            peer_onward(q).start()

            @pl.when(j >= half_rows)
            def _():
                peer_across(q).start()

            convert(peer, q, own_at, 1 - y)

        @pl.when((lead == 0) & (j >= half_rows))
        def _():
            landed(peer_across, q)
            convert(sibp, q, sib_at, 1 - y)

    def early(j):
        q = at(j)

        @pl.when(j < rows - 2)
        def _():
            left_arrive(j)

        @pl.when((j == TRIGGER) & (lead == 0))
        def _():
            each(0, rows, lambda i: to_peer(i).start())

        @pl.when((lead == 0) | (j < half_rows))
        def _():
            landed(halo_across, q)

            @pl.when((lead == 0) & (j < half_rows))
            def _():
                halo_across(q).start()

            convert(halo, q, halo_at, y)

        @pl.when((lead == 1) | (j >= half_rows))
        def _():
            landed(own_across, q)
            convert(sib, q, sib_at, y)

    each(0, rows, early)
    fetch.wait()

    halo_early = pairs - 1 - lead * (pairs // 2 - 1)
    late_at = own_at + (sib_at - own_at) * lead
    early_at = sib_at + (own_at - sib_at) * lead
    early_first = pairs // 2 * (1 - lead)
    halo_lag = pairs // 2 * lead
    most = half_rows - 1

    def late_pair(k, first, last):
        pair_rows(
            late_at + left_order(2 * k, y), late_at + left_order(2 * k + 1, y), first, last
        )

    def halo_pair(k, first, last):
        near_pair(halo_at + lower(k), first, last)

    def one_step(step):
        first, last = 1 - y, most + 1 - y
        onward_arrive(2 * step)

        @pl.when((step == pairs - 1) & (lead == 1))
        def _():
            each(rows - 2, rows, lambda i: to_peer(i).start())

        @pl.when(step < pairs - 1)
        def _():
            late_pair(step, first, last)

        onward_arrive(2 * step + 1)

        fresh = step - halo_lag

        @pl.when((fresh >= 0) & (fresh < halo_early))
        def _():
            halo_arrive(2 * fresh)
            halo_arrive(2 * fresh + 1)
            halo_pair(fresh, first, last)

        @pl.when(step >= early_first)
        def _():
            near_pair(early_at + lower(step), first, last)

    each(0, pairs, one_step)
    left_arrive(rows - 2)
    left_arrive(rows - 1)

    def finish(n):
        row = row_at(n)

        @pl.when(n == most)
        def _():
            each(early_first, pairs, lambda k: near_pair(early_at + lower(k), row, row + 1))
            each(0, pairs - 1, lambda k: late_pair(k, row, row + 1))
            each(0, halo_early, lambda k: halo_pair(k, row, row + 1))

        @pl.when((n == half_rows // 2) & (lead == 0))
        def _():
            halo_arrive(rows - 2)
            halo_arrive(rows - 1)

        @pl.when(lead == 0)
        def _():
            halo_pair(pairs - 1, row, row + 1)

        late_pair(pairs - 1, row, row + 1)
        cube(n)

    each(0, half_rows, finish)

    for copy in column_copies:
        copy.wait_send()
    each(0, rows, lambda j: to_peer(j).wait_send())

    @pl.when(lead == 0)
    def _():
        each(0, half_rows, lambda j: halo_across(at(j)).wait_send())
        each(0, half_rows, lambda j: halop_across(at(j)).wait_send())
        each(0, rows, lambda j: own_across(at(j)).wait_send())
        each(0, rows, lambda j: peer_across(at(j)).wait_send())

    @pl.when(lead == 1)
    def _():
        each(0, rows, lambda j: own_onward(at(j)).wait_send())
        each(0, rows, lambda j: peer_onward(at(j)).wait_send())
        each(half_rows, rows, lambda j: own_across(at(j)).wait_send())
        each(half_rows, rows, lambda j: peer_across(at(j)).wait_send())

    send_kept(half_rows - 1)

    def out_landed(q):
        remote(
            square.at[pl.ds(0, width)], result.at[q], osend.at[0, 0], orecv.at[q], r, 1 - y
        ).wait_recv()

    each(0, half_rows, lambda n: across_out(n).wait_send())

    @pl.when(lead == 0)
    def _():
        each(0, half_rows, lambda n: kept_out(n).wait())
        each(0, half_rows, lambda n: out_landed(half_rows - first_row + n))

    @pl.when(lead == 1)
    def _():
        each(0, half_rows, lambda n: sibling_out(n).wait_send())
        each(0, rows, out_landed)


def paired(density, columns):
    rows, width, order, _ = density.shape
    slots = 2 * width
    frames = 2 * rows + rows // 2
    blocks = frames * slots
    targets = rows // 2 * slots
    lanes = 128
    padded = jnp.where(
        lax.axis_index("col") == 0,
        jnp.pad(columns, ((0, 0), (0, lanes - width))),
        jnp.pad(columns, ((0, 0), (width, lanes - slots))),
    )
    any_spec = pl.BlockSpec(memory_space=pl.ANY)
    vmem_spec = pl.BlockSpec(memory_space=pltpu.VMEM)
    landing = pltpu.VMEM((rows, width, order, order), jnp.float32)
    return pl.pallas_call(
        fused_kernel,
        out_shape=jax.ShapeDtypeStruct((rows, width, order, order), jnp.float32),
        in_specs=[any_spec, vmem_spec],
        out_specs=any_spec,
        scratch_shapes=[landing] * 6
        + [
            pltpu.VMEM((blocks + 1, order, 2 * order), jnp.bfloat16),
            pltpu.VMEM((targets, order, order), jnp.float32),
            pltpu.VMEM((slots, 2 * order, order), jnp.bfloat16),
            pltpu.VMEM((6, rows, lanes), jnp.int32),
            pltpu.VMEM((3 * rows, lanes), jnp.int32),
            pltpu.VMEM((rows // 2, 3 * rows + 8, lanes), jnp.int32),
            pltpu.SMEM((rows // 2, 3 * rows + 8, lanes), jnp.int32),
            pltpu.SemaphoreType.DMA,
            pltpu.SemaphoreType.DMA((5, rows)),
            pltpu.SemaphoreType.DMA((5, rows)),
            pltpu.SemaphoreType.DMA((5,)),
            pltpu.SemaphoreType.DMA((6,)),
            pltpu.SemaphoreType.DMA,
            pltpu.SemaphoreType.DMA((2, rows // 2)),
            pltpu.SemaphoreType.DMA((rows,)),
        ],
        compiler_params=pltpu.CompilerParams(
            vmem_limit_bytes=62 * 1024 * 1024, collective_id=0, has_side_effects=True
        ),
        cost_estimate=pl.CostEstimate(
            flops=16 * targets * slots * order**3,
            bytes_accessed=blocks * order * order * 4,
            transcendentals=0,
        ),
    )(density, padded)


def per_device(density, columns):
    local_rows, local_slots, order, _ = density.shape
    row_count = lax.axis_size("row")
    column_count = lax.axis_size("col")
    slots = local_slots * column_count
    if column_count == 2 and local_rows == W and row_count % 2 == 0 and row_count >= 6:
        return paired(density, columns)
    rows = local_rows // column_count
    block_count = local_rows * row_count
    row_start = lax.axis_index("row") * local_rows
    column = lax.axis_index("col")
    own_start = column * rows
    if column_count == 2:
        numbers = range(2 * row_count)
        around = 2 * row_count

        def from_row(step):
            same = [(i, (i - 2 * step) % around) for i in numbers]
            cross = [(i, ((i ^ 1) - 2 * step) % around) for i in numbers]
            mine = lax.ppermute(columns, ("row", "col"), same) if step else columns
            peer = lax.ppermute(columns, ("row", "col"), cross)
            return mine, peer

        parts = [from_row(step) for step in (-1, 0, 1)]
        density, parts = lax.optimization_barrier((density, parts))
        before, full_columns, after = [
            jnp.where(
                column == 0,
                jnp.concatenate([mine, peer], axis=1),
                jnp.concatenate([peer, mine], axis=1),
            )
            for mine, peer in parts
        ]
    else:
        full_columns = lax.all_gather(columns, "col", axis=1, tiled=True)
        before = shifted(full_columns, 1)
        after = shifted(full_columns, -1)
    ext_columns = jnp.concatenate([before[local_rows - W :], full_columns, after[:W]])
    trimmed = column_count == 2 and local_rows == W
    panel_start = own_start if trimmed else 0
    total, *lists = work_lists(
        ext_columns, own_start, panel_start, row_start, block_count, rows
    )
    if trimmed:
        ring = [(2 * i, 2 * ((i + 1) % row_count)) for i in range(row_count)]
        back = [(2 * ((i + 1) % row_count) + 1, 2 * i + 1) for i in range(row_count)]
        far_pairs = ring + back
        near_pairs = [(b, a) for a, b in far_pairs]
        peers = [(i, i ^ 1) for i in range(2 * row_count)]
        axes = ("row", "col")
        near_at = column * rows
        rest_at = (1 - column) * rows
        own_near = lax.dynamic_slice_in_dim(density, near_at, rows)
        own_rest = lax.dynamic_slice_in_dim(density, rest_at, rows)
        other_near = lax.ppermute(own_rest, axes, peers)
        far_own = lax.ppermute(density, axes, far_pairs)
        near_own = lax.ppermute(own_near, axes, near_pairs)
        second, other_near = lax.optimization_barrier((own_near, other_near))
        other_rest = lax.ppermute(second, axes, peers)
        near_other = lax.ppermute(other_near, axes, near_pairs)
        far_other_near = lax.ppermute(other_near, axes, far_pairs)
        far_other_rest = lax.ppermute(other_rest, axes, far_pairs)
        pieces = [
            density,
            far_own,
            near_own,
            other_near,
            other_rest,
            near_other,
            far_other_near,
            far_other_rest,
        ]
        own_row = W - own_start
        far_row = jnp.where(column == 0, 0, rows + local_rows)
        near_row = jnp.where(column == 0, W + local_rows, 0)
        here = column * local_slots
        there = (1 - column) * local_slots
        firsts = [
            own_row * slots + here,
            far_row * slots + here,
            near_row * slots + here,
            (own_row + near_at) * slots + there,
            (own_row + rest_at) * slots + there,
            near_row * slots + there,
            (far_row + near_at) * slots + there,
            (far_row + rest_at) * slots + there,
        ]
        panel_rows = 2 * W + rows
    else:
        full_rows = lax.all_gather(density, "col", axis=1, tiled=True)
        pieces = [
            shifted(full_rows[local_rows - W :], 1),
            full_rows,
            shifted(full_rows[:W], -1),
        ]
        firsts = [0, W * slots, (W + local_rows) * slots]
        panel_rows = 2 * W + local_rows
    left_base = (W + own_start - panel_start) * slots
    result = products(total, left_base, firsts, lists, pieces, panel_rows, slots, rows)
    result = result.reshape(rows, slots, order, order)
    if column_count != 2:
        return lax.all_to_all(result, "col", split_axis=1, concat_axis=0, tiled=True)
    kept = lax.dynamic_slice_in_dim(result, column * local_slots, local_slots, axis=1)
    sent = lax.dynamic_slice_in_dim(result, (1 - column) * local_slots, local_slots, axis=1)
    arrived = lax.ppermute(sent, "col", [(0, 1), (1, 0)])
    return jnp.where(
        column == 0,
        jnp.concatenate([kept, arrived]),
        jnp.concatenate([arrived, kept]),
    )


def solution(mesh):
    in_specs = (P("row", "col", None, None), P("row", "col"))
    out_specs = P("row", "col", None, None)
    return jax.shard_map(
        per_device, mesh=mesh, in_specs=in_specs, out_specs=out_specs, check_vma=False
    )
```

```python
import functools

import jax
import jax.numpy as jnp
from jax import lax
from jax.experimental import pallas as pl
from jax.experimental.pallas import tpu as pltpu
from jax.sharding import PartitionSpec as P

W = 8
GROUP = 4
UNROLL = 2
SPAN = 8
TRIGGER = 4


def shifted(value, step):
    count = lax.axis_size("row")
    return lax.ppermute(value, "row", [(i, (i + step) % count) for i in range(count)])


def work_lists(ext_columns, own_start, panel_start, row_start, block_count, rows):
    slots = ext_columns.shape[1]
    own = lax.dynamic_slice_in_dim(ext_columns, W + own_start, rows)
    row_ids = jnp.arange(rows, dtype=jnp.int32)[:, None]
    offset = (own - (row_start + own_start + row_ids) + W) % block_count - W
    ext_row = jnp.where(own >= 0, W + own_start + row_ids + offset, 0)
    candidate = ext_columns[ext_row]
    matched = (
        (candidate[:, None] == own[:, :, None, None])
        & (own >= 0)[:, :, None, None]
        & (own >= 0)[:, None, :, None]
    )
    present = jnp.any(matched, axis=-1)
    slot_ids = jnp.arange(slots, dtype=jnp.int32)
    picked = jnp.sum(jnp.where(matched, slot_ids, 0), axis=-1)
    right = jnp.where(present, (ext_row - panel_start)[:, None, :] * slots + picked, 0)
    left = jnp.broadcast_to((row_ids * slots + slot_ids)[:, None, :], present.shape)
    targets = rows * slots
    present = present.reshape(targets, slots)
    rank = jnp.cumsum(present.astype(jnp.int32), axis=-1) - 1
    counts = jnp.sum(present.astype(jnp.int32), axis=-1)
    chosen = present[:, :, None] & (rank[:, :, None] == slot_ids)
    filled = slot_ids < counts[:, None]
    left_list = jnp.sum(jnp.where(chosen, left.reshape(targets, slots)[:, :, None], 0), axis=1)
    left_list = jnp.where(filled, left_list, targets)
    right_list = jnp.sum(jnp.where(chosen, right.reshape(targets, slots)[:, :, None], 0), axis=1)
    per_target = slots // GROUP
    chunks = (counts + GROUP - 1) // GROUP
    ends = jnp.cumsum(chunks)
    total = ends[-1]
    turns = jnp.arange(targets * per_target, dtype=jnp.int32)
    target = jnp.minimum(
        jnp.sum((ends[None, :] <= turns[:, None]).astype(jnp.int32), axis=1), targets - 1
    )
    place = jnp.clip(turns - (ends - chunks)[target], 0, per_target - 1)
    at = target * per_target + place
    live = (turns < total)[:, None]
    left_chunks = jnp.where(live, left_list.reshape(-1, GROUP)[at], targets)
    right_chunks = jnp.where(live, right_list.reshape(-1, GROUP)[at], 0)
    return total, target, left_chunks.reshape(-1), right_chunks.reshape(-1)


def split(value):
    high = value.astype(jnp.bfloat16)
    low = (value - high.astype(jnp.float32)).astype(jnp.bfloat16)
    return high, low


def kernel(sizes, slots, targets, meta, target_list, left_list, right_list, *refs):
    pieces = refs[: len(sizes)]
    out, stage, panel, left, square, sems = refs[len(sizes) :]
    order = out.shape[-1]
    starts = []
    at = 0
    for rows, width in sizes:
        starts.append(at)
        at += rows * width
    copies = [
        pltpu.make_async_copy(
            piece, stage.at[pl.ds(start, rows * width)], sems.at[number]
        )
        for number, (piece, start, (rows, width)) in enumerate(zip(pieces, starts, sizes))
    ]
    for copy in copies:
        copy.start()
    left[targets] = jnp.zeros((2 * order, order), jnp.bfloat16)

    def clear(block, carry):
        square[block] = jnp.zeros((order, order), jnp.float32)
        return carry

    lax.fori_loop(0, targets, clear, 0)
    for number, (copy, start, (rows, width)) in enumerate(zip(copies, starts, sizes)):
        copy.wait()
        first = meta[2 + number]

        def place(block, carry, start=start, width=width, first=first):
            high, low = split(stage[start + block])
            where = first + (block // width) * slots + block % width
            panel[where, :, :order] = high
            panel[where, :, order:] = low
            return carry

        lax.fori_loop(0, rows * width, place, 0)
    left_base = meta[1]

    def load_left(block, carry):
        left[block, :order] = panel[left_base + block, :, :order]
        left[block, order:] = panel[left_base + block, :, order:]
        return carry

    lax.fori_loop(0, targets, load_left, 0)
    rounds = (meta[0] + UNROLL - 1) // UNROLL

    def product(result, factor):
        def step(turn, carry):
            sums = []
            for inner in range(UNROLL):
                begin = (turn * UNROLL + inner) * GROUP
                lhs = jnp.concatenate([left[left_list[begin + g]] for g in range(GROUP)], axis=1)
                rhs = jnp.concatenate([panel[right_list[begin + g]] for g in range(GROUP)], axis=0)
                both = jnp.dot(lhs, rhs, preferred_element_type=jnp.float32)
                sums.append(
                    both[:order, :order]
                    + (both[:order, order:] + both[order:, :order])
                    + both[order:, order:]
                )
            for inner in range(UNROLL):
                target = target_list[turn * UNROLL + inner]
                result[target] += sums[inner] if factor == 1.0 else factor * sums[inner]
            return carry

        lax.fori_loop(0, rounds, step, 0)

    product(square, 1.0)

    def middle(block, carry):
        value = square[block]
        high, low = split(value)
        left[block, :order] = high
        left[block, order:] = low
        out[block] = 3.0 * value
        return carry

    lax.fori_loop(0, targets, middle, 0)
    product(out, -2.0)


def products(total, left_base, firsts, lists, pieces, panel_rows, slots, rows):
    order = pieces[0].shape[-1]
    sizes = tuple((piece.shape[0], piece.shape[1]) for piece in pieces)
    targets = rows * slots
    meta = jnp.stack([jnp.asarray(v, jnp.int32) for v in (total, left_base, *firsts)])
    blocks = sum(a * b for a, b in sizes)
    any_spec = pl.BlockSpec(memory_space=pl.ANY)
    smem_spec = pl.BlockSpec(memory_space=pltpu.SMEM)
    return pl.pallas_call(
        functools.partial(kernel, sizes, slots, targets),
        out_shape=jax.ShapeDtypeStruct((targets, order, order), jnp.float32),
        in_specs=[smem_spec] * 4 + [any_spec] * len(pieces),
        out_specs=pl.BlockSpec(memory_space=pltpu.VMEM),
        scratch_shapes=[
            pltpu.VMEM((blocks, order, order), jnp.float32),
            pltpu.VMEM((panel_rows * slots, order, 2 * order), jnp.bfloat16),
            pltpu.VMEM((targets + 1, 2 * order, order), jnp.bfloat16),
            pltpu.VMEM((targets, order, order), jnp.float32),
            pltpu.SemaphoreType.DMA((len(pieces),)),
        ],
        compiler_params=pltpu.CompilerParams(vmem_limit_bytes=62 * 1024 * 1024),
        cost_estimate=pl.CostEstimate(
            flops=8 * targets * 8 * order**3,
            bytes_accessed=blocks * order * order * 4,
            transcendentals=0,
        ),
    )(meta, *lists, *[piece.reshape(-1, order, order) for piece in pieces])


MESH = pl.DeviceIdType.MESH


def fused_kernel(
    dens, cols, result,
    own, peer, halo, halop, sib, sibp, stage, square, left, listed, lanes_ref, table, index,
    own_sem, ssem, rsem, csend, crecv, table_sem, osend, orecv,
):
    rows, width = dens.shape[0], dens.shape[1]
    order = dens.shape[-1]
    slots = 2 * width
    half_rows = rows // 2
    pairs = rows // 2
    targets = square.shape[0]
    nothing = stage.shape[0] - 1
    count = lax.axis_size("row")
    block_count = count * rows
    r = lax.axis_index("row")
    y = lax.axis_index("col")
    core = r % 2
    lead = (core + y) % 2
    sibling = r + 1 - 2 * core
    side = 1 - 2 * y
    onward = (r + side + count) % count
    turn = 2 * core - 1
    near_row = (r + turn + count) % count
    next_row = (r + 2 * turn + count) % count
    from_row = (r - core - 1 + 3 * y + count) % count

    barrier = pltpu.get_barrier_semaphore()
    for row, column in (
        (r, 1 - y), (sibling, y), (sibling, 1 - y), (from_row, y), (from_row, 1 - y)
    ):
        pl.semaphore_signal(barrier, inc=1, device_id=(row, column), device_id_type=MESH)
    own_copy = pltpu.make_async_copy(dens, own, own_sem)
    own_copy.start()
    pl.semaphore_wait(barrier, 5)

    def remote(src, dst, send, recv, row, column):
        return pltpu.make_async_remote_copy(
            src_ref=src, dst_ref=dst, send_sem=send, recv_sem=recv,
            device_id=(row, column), device_id_type=MESH,
        )

    mine = (core + 1 - y) * 2 + y
    column_copies = [
        remote(cols, listed.at[place], csend.at[number], crecv.at[place], row, column)
        for number, (row, column, place) in enumerate((
            (r, 1 - y, (core + y) * 2 + y),
            (sibling, y, (core + 1 - y) * 2 + y),
            (sibling, 1 - y, (core + y) * 2 + y),
            (near_row, 1 - core, 2 * (1 - core) * 2 + y),
            (next_row, 1 - core, 2 * (1 - core) * 2 + y),
        ))
    ]

    def order_of(j, plane):
        back = rows - 2 - 2 * (j // 2) + j % 2
        return back + (j - back) * plane

    def at(j):
        return order_of(j, y)

    def left_order(j, plane):
        n = j // 2
        back = half_rows - 1 - n
        return back + (n - back) * plane + half_rows * (j % 2)

    def to_peer(j):
        early, late = order_of(j, 1 - y), left_order(j, 1 - y)
        q = early + (late - early) * lead
        return remote(dens.at[q], peer.at[q], ssem.at[0, q], rsem.at[0, q], r, 1 - y)

    def own_onward(q):
        return remote(dens.at[q], halo.at[q], ssem.at[1, q], rsem.at[1, q], onward, y)

    def peer_onward(q):
        return remote(peer.at[q], halop.at[q], ssem.at[2, q], rsem.at[2, q], onward, y)

    def halo_across(q):
        return remote(halo.at[q], halo.at[q], ssem.at[1, q], rsem.at[1, q], sibling, y)

    def halop_across(q):
        return remote(halop.at[q], halop.at[q], ssem.at[2, q], rsem.at[2, q], sibling, y)

    def own_across(q):
        return remote(dens.at[q], sib.at[q], ssem.at[3, q], rsem.at[3, q], sibling, y)

    def peer_across(q):
        return remote(peer.at[q], sibp.at[q], ssem.at[4, q], rsem.at[4, q], sibling, y)

    def each(low, high, body):
        def step(j, carry):
            body(j)
            return carry

        lax.fori_loop(low, high, step, 0)

    own_at = (8 + 4 * lead - y * (4 + 8 * lead)) * half_rows // 4
    halo_at = (-4 * lead + y * (12 + 8 * lead)) * half_rows // 4
    sib_at = (16 - 12 * lead + y * (-20 + 24 * lead)) * half_rows // 4

    def convert(source, q, first, half):
        def block(b, carry):
            high, low = split(source[q, b])
            where = (first + q) * slots + half * width + b
            stage[where, :, :order] = high
            stage[where, :, order:] = low
            return carry

        lax.fori_loop(0, width, block, 0)

    for copy in column_copies:
        copy.start()

    @pl.when(lead == 1)
    def _():
        each(0, rows - 2, lambda j: to_peer(j).start())
        each(0, rows, lambda j: own_onward(at(j)).start())

    listed[mine] = cols[...]

    @pl.when(lead == 0)
    def _():
        each(0, rows, lambda j: own_across(at(j)).start())

    @pl.when(lead == 1)
    def _():
        each(half_rows, rows, lambda j: own_across(at(j)).start())

    stage[nothing] = jnp.zeros((order, 2 * order), jnp.bfloat16)

    def clear(block, carry):
        square[block] = jnp.zeros((order, order), jnp.float32)
        return carry

    lax.fori_loop(0, targets, clear, 0)

    for number, place in enumerate((
        (core + 1 - y) * 2 + 1 - y,
        (2 - core - y) * 2 + y,
        (2 - core - y) * 2 + 1 - y,
        2 * y * 2 + y,
        2 * y * 2 + 1 - y,
    )):
        remote(cols, listed.at[place], csend.at[number], crecv.at[place], r, 1 - y).wait_recv()
    for group in range(3):
        lanes_ref[group * rows : (group + 1) * rows] = listed[2 * group] + listed[2 * group + 1]
    reach = lanes_ref[...]
    grid = reach.shape
    shift = half_rows * core
    base = ((r - core) * rows - W * (1 - y) + block_count) % block_count
    lane = lax.broadcasted_iota(jnp.int32, grid, 1)
    line = lax.broadcasted_iota(jnp.int32, grid, 0)
    absolute = base + line
    absolute = jnp.where(absolute >= block_count, absolute - block_count, absolute)
    staged = (line >= shift) & (line < shift + nothing // slots)
    for row in range(half_rows):
        goal = jnp.broadcast_to(lanes_ref[pl.ds(W + row + shift, 1)], grid)
        goal = jnp.where((lane < slots) & (goal >= 0), goal, -2)
        right = jnp.full(grid, nothing, jnp.int32)
        from_left = jnp.full(grid, nothing, jnp.int32)
        for slot in range(slots):
            held = jnp.broadcast_to(reach[:, slot : slot + 1], grid)
            right = jnp.where((held == goal) & staged, (line - shift) * slots + slot, right)
            wanted = jnp.broadcast_to(goal[:, slot : slot + 1], grid)
            from_left = jnp.where(wanted == absolute, (W + row) * slots + slot, from_left)
        table[row, : grid[0]] = jnp.where(lane < 64, right, from_left)
        away = goal - base
        away = jnp.where(away < 0, away + block_count, away)
        usable = (goal >= 0) & (away >= shift) & (away < shift + nothing // slots)
        away = jnp.where(usable, away, shift)
        table[row, grid[0] : grid[0] + 8] = away[:8]
    fetch = pltpu.make_async_copy(table, index, table_sem)
    fetch.start()

    own_copy.wait()
    each(0, rows, lambda q: convert(own, q, own_at, y))

    def quarters(both):
        return (
            both[:order, :order]
            + (both[:order, order:] + both[order:, :order])
            + both[order:, order:]
        )

    def reaching(frame):
        return jnp.maximum(frame - 2 * W, 0), jnp.minimum(frame + 2, half_rows)

    def near_pair(frame, first, last):
        low, high = reaching(frame)
        pair_rows(frame, frame + 1, jnp.maximum(low, first), jnp.minimum(high, last))

    def pair_rows(frame, other, low, high):
        def one_row(row, carry):
            one = stage[index[row, frame + shift, 64]]
            two = stage[index[row, other + shift, 64]]
            lhs = jnp.concatenate(
                [
                    jnp.concatenate([one[:, :order], two[:, :order]], axis=1),
                    jnp.concatenate([one[:, order:], two[:, order:]], axis=1),
                ],
                axis=0,
            )

            def some(step, carry):
                sums = []
                for inner in range(SPAN):
                    slot = step * SPAN + inner
                    rhs = jnp.concatenate(
                        [
                            stage[index[row, frame + shift, slot]],
                            stage[index[row, other + shift, slot]],
                        ],
                        axis=0,
                    )
                    sums.append(quarters(jnp.dot(lhs, rhs, preferred_element_type=jnp.float32)))
                for inner in range(SPAN):
                    square[row * slots + step * SPAN + inner] += sums[inner]
                return carry

            return lax.fori_loop(0, slots // SPAN, some, carry)

        lax.fori_loop(low, high, one_row, 0)

    holder = r + (sibling - r) * lead
    first_row = half_rows * core

    def row_at(n):
        return half_rows - 1 - n + y * (2 * n + 1 - half_rows)

    def across_out(n):
        row = row_at(n)
        half = 1 - y
        return remote(
            square.at[pl.ds(row * slots + half * width, width)],
            result.at[first_row + row],
            osend.at[0, row], orecv.at[first_row + row], holder, 1 - y,
        )

    def kept_out(n):
        row = row_at(n)
        return pltpu.make_async_copy(
            square.at[pl.ds(row * slots + y * width, width)],
            result.at[first_row + row],
            osend.at[1, row],
        )

    def sibling_out(n):
        row = row_at(n)
        return remote(
            square.at[pl.ds(row * slots + y * width, width)],
            result.at[first_row + row],
            osend.at[1, row], orecv.at[first_row + row], sibling, y,
        )

    def send_kept(n):
        @pl.when(lead == 0)
        def _():
            kept_out(n).start()

        @pl.when(lead == 1)
        def _():
            sibling_out(n).start()

    def cube(n):
        row = row_at(n)

        def middle(slot, carry):
            high, low = split(square[row * slots + slot])
            left[slot, :order] = high
            left[slot, order:] = low
            return carry

        lax.fori_loop(0, slots, middle, 0)

        @pl.when(n > 0)
        def _():
            send_kept(n - 1)

        lines = [index[row, 3 * rows, slot] for slot in range(slots)]

        def one_target(step, carry):
            slot = (step + width * (1 - y)) % slots
            both = None
            for group in range(slots // GROUP):
                members = range(group * GROUP, (group + 1) * GROUP)
                lhs = jnp.concatenate([left[m] for m in members], axis=1)
                rhs = jnp.concatenate(
                    [stage[index[row, lines[m], slot]] for m in members], axis=0
                )
                part = jnp.dot(lhs, rhs, preferred_element_type=jnp.float32)
                both = part if both is None else both + part
            where = row * slots + slot
            square[where] = 3.0 * square[where] - 2.0 * quarters(both)

            @pl.when(step == width)
            def _():
                across_out(n).start()

            return carry

        lax.fori_loop(0, slots, one_target, 0)

    def landed(make, q):
        make(q).wait_recv()

    def peer_landed(q):
        remote(peer.at[q], peer.at[q], ssem.at[0, q], rsem.at[0, q], r, 1 - y).wait_recv()

    def lower(k):
        return at(2 * k)

    def halo_arrive(j):
        q = at(j)
        landed(halop_across, q)

        @pl.when(j < half_rows * (1 - lead))
        def _():
            halop_across(q).start()

        convert(halop, q, halo_at, 1 - y)

    def left_arrive(j):
        q = left_order(j, y)

        @pl.when(lead == 0)
        def _():
            peer_landed(q)
            peer_across(q).start()
            convert(peer, q, own_at, 1 - y)

        @pl.when(lead == 1)
        def _():
            landed(peer_across, q)
            convert(sibp, q, sib_at, 1 - y)

    def onward_arrive(j):
        q = at(j)

        @pl.when(lead == 1)
        def _():
            peer_landed(q)
            peer_onward(q).start()

            @pl.when(j >= half_rows)
            def _():
                peer_across(q).start()

            convert(peer, q, own_at, 1 - y)

        @pl.when((lead == 0) & (j >= half_rows))
        def _():
            landed(peer_across, q)
            convert(sibp, q, sib_at, 1 - y)

    def early(j):
        q = at(j)

        @pl.when(j < rows - 2)
        def _():
            left_arrive(j)

        @pl.when((j == TRIGGER) & (lead == 0))
        def _():
            each(0, rows, lambda i: to_peer(i).start())

        @pl.when((lead == 0) | (j < half_rows))
        def _():
            landed(halo_across, q)

            @pl.when((lead == 0) & (j < half_rows))
            def _():
                halo_across(q).start()

            convert(halo, q, halo_at, y)

        @pl.when((lead == 1) | (j >= half_rows))
        def _():
            landed(own_across, q)
            convert(sib, q, sib_at, y)

    each(0, rows, early)
    fetch.wait()

    halo_early = pairs - 1 - lead * (pairs // 2 - 1)
    late_at = own_at + (sib_at - own_at) * lead
    early_at = sib_at + (own_at - sib_at) * lead
    early_first = pairs // 2 * (1 - lead)
    halo_lag = pairs // 2 * lead
    most = half_rows - 1

    def late_pair(k, first, last):
        pair_rows(
            late_at + left_order(2 * k, y), late_at + left_order(2 * k + 1, y), first, last
        )

    def halo_pair(k, first, last):
        near_pair(halo_at + lower(k), first, last)

    def one_step(step):
        first, last = 1 - y, most + 1 - y
        onward_arrive(2 * step)

        @pl.when((step == pairs - 1) & (lead == 1))
        def _():
            each(rows - 2, rows, lambda i: to_peer(i).start())

        @pl.when(step < pairs - 1)
        def _():
            late_pair(step, first, last)

        onward_arrive(2 * step + 1)

        fresh = step - halo_lag

        @pl.when((fresh >= 0) & (fresh < halo_early))
        def _():
            halo_arrive(2 * fresh)
            halo_arrive(2 * fresh + 1)
            halo_pair(fresh, first, last)

        @pl.when(step >= early_first)
        def _():
            near_pair(early_at + lower(step), first, last)

    each(0, pairs, one_step)
    left_arrive(rows - 2)
    left_arrive(rows - 1)

    def finish(n):
        row = row_at(n)

        @pl.when(n == most)
        def _():
            each(early_first, pairs, lambda k: near_pair(early_at + lower(k), row, row + 1))
            each(0, pairs - 1, lambda k: late_pair(k, row, row + 1))
            each(0, halo_early, lambda k: halo_pair(k, row, row + 1))

        @pl.when((n == half_rows // 2) & (lead == 0))
        def _():
            halo_arrive(rows - 2)
            halo_arrive(rows - 1)

        @pl.when(lead == 0)
        def _():
            halo_pair(pairs - 1, row, row + 1)

        late_pair(pairs - 1, row, row + 1)
        cube(n)

    each(0, half_rows, finish)

    for copy in column_copies:
        copy.wait_send()
    each(0, rows, lambda j: to_peer(j).wait_send())

    @pl.when(lead == 0)
    def _():
        each(0, half_rows, lambda j: halo_across(at(j)).wait_send())
        each(0, half_rows, lambda j: halop_across(at(j)).wait_send())
        each(0, rows, lambda j: own_across(at(j)).wait_send())
        each(0, rows, lambda j: peer_across(at(j)).wait_send())

    @pl.when(lead == 1)
    def _():
        each(0, rows, lambda j: own_onward(at(j)).wait_send())
        each(0, rows, lambda j: peer_onward(at(j)).wait_send())
        each(half_rows, rows, lambda j: own_across(at(j)).wait_send())
        each(half_rows, rows, lambda j: peer_across(at(j)).wait_send())

    send_kept(half_rows - 1)

    def out_landed(q):
        remote(
            square.at[pl.ds(0, width)], result.at[q], osend.at[0, 0], orecv.at[q], r, 1 - y
        ).wait_recv()

    each(0, half_rows, lambda n: across_out(n).wait_send())

    @pl.when(lead == 0)
    def _():
        each(0, half_rows, lambda n: kept_out(n).wait())
        each(0, half_rows, lambda n: out_landed(half_rows - first_row + n))

    @pl.when(lead == 1)
    def _():
        each(0, half_rows, lambda n: sibling_out(n).wait_send())
        each(0, rows, out_landed)


def paired(density, columns):
    rows, width, order, _ = density.shape
    slots = 2 * width
    frames = 2 * rows + rows // 2
    blocks = frames * slots
    targets = rows // 2 * slots
    lanes = 128
    padded = jnp.where(
        lax.axis_index("col") == 0,
        jnp.pad(columns, ((0, 0), (0, lanes - width))),
        jnp.pad(columns, ((0, 0), (width, lanes - slots))),
    )
    any_spec = pl.BlockSpec(memory_space=pl.ANY)
    vmem_spec = pl.BlockSpec(memory_space=pltpu.VMEM)
    landing = pltpu.VMEM((rows, width, order, order), jnp.float32)
    return pl.pallas_call(
        fused_kernel,
        out_shape=jax.ShapeDtypeStruct((rows, width, order, order), jnp.float32),
        in_specs=[any_spec, vmem_spec],
        out_specs=any_spec,
        scratch_shapes=[landing] * 6
        + [
            pltpu.VMEM((blocks + 1, order, 2 * order), jnp.bfloat16),
            pltpu.VMEM((targets, order, order), jnp.float32),
            pltpu.VMEM((slots, 2 * order, order), jnp.bfloat16),
            pltpu.VMEM((6, rows, lanes), jnp.int32),
            pltpu.VMEM((3 * rows, lanes), jnp.int32),
            pltpu.VMEM((rows // 2, 3 * rows + 8, lanes), jnp.int32),
            pltpu.SMEM((rows // 2, 3 * rows + 8, lanes), jnp.int32),
            pltpu.SemaphoreType.DMA,
            pltpu.SemaphoreType.DMA((5, rows)),
            pltpu.SemaphoreType.DMA((5, rows)),
            pltpu.SemaphoreType.DMA((5,)),
            pltpu.SemaphoreType.DMA((6,)),
            pltpu.SemaphoreType.DMA,
            pltpu.SemaphoreType.DMA((2, rows // 2)),
            pltpu.SemaphoreType.DMA((rows,)),
        ],
        compiler_params=pltpu.CompilerParams(
            vmem_limit_bytes=62 * 1024 * 1024, collective_id=0, has_side_effects=True
        ),
        cost_estimate=pl.CostEstimate(
            flops=16 * targets * slots * order**3,
            bytes_accessed=blocks * order * order * 4,
            transcendentals=0,
        ),
    )(density, padded)


def per_device(density, columns):
    local_rows, local_slots, order, _ = density.shape
    row_count = lax.axis_size("row")
    column_count = lax.axis_size("col")
    slots = local_slots * column_count
    if column_count == 2 and local_rows == W and row_count % 2 == 0 and row_count >= 6 and slots % SPAN == 0:
        return paired(density, columns)
    rows = local_rows // column_count
    block_count = local_rows * row_count
    row_start = lax.axis_index("row") * local_rows
    column = lax.axis_index("col")
    own_start = column * rows
    if column_count == 2:
        numbers = range(2 * row_count)
        around = 2 * row_count

        def from_row(step):
            same = [(i, (i - 2 * step) % around) for i in numbers]
            cross = [(i, ((i ^ 1) - 2 * step) % around) for i in numbers]
            mine = lax.ppermute(columns, ("row", "col"), same) if step else columns
            peer = lax.ppermute(columns, ("row", "col"), cross)
            return mine, peer

        parts = [from_row(step) for step in (-1, 0, 1)]
        density, parts = lax.optimization_barrier((density, parts))
        before, full_columns, after = [
            jnp.where(
                column == 0,
                jnp.concatenate([mine, peer], axis=1),
                jnp.concatenate([peer, mine], axis=1),
            )
            for mine, peer in parts
        ]
    else:
        full_columns = lax.all_gather(columns, "col", axis=1, tiled=True)
        before = shifted(full_columns, 1)
        after = shifted(full_columns, -1)
    ext_columns = jnp.concatenate([before[local_rows - W :], full_columns, after[:W]])
    trimmed = column_count == 2 and local_rows == W
    panel_start = own_start if trimmed else 0
    total, *lists = work_lists(
        ext_columns, own_start, panel_start, row_start, block_count, rows
    )
    if trimmed:
        ring = [(2 * i, 2 * ((i + 1) % row_count)) for i in range(row_count)]
        back = [(2 * ((i + 1) % row_count) + 1, 2 * i + 1) for i in range(row_count)]
        far_pairs = ring + back
        near_pairs = [(b, a) for a, b in far_pairs]
        peers = [(i, i ^ 1) for i in range(2 * row_count)]
        axes = ("row", "col")
        near_at = column * rows
        rest_at = (1 - column) * rows
        own_near = lax.dynamic_slice_in_dim(density, near_at, rows)
        own_rest = lax.dynamic_slice_in_dim(density, rest_at, rows)
        other_near = lax.ppermute(own_rest, axes, peers)
        far_own = lax.ppermute(density, axes, far_pairs)
        near_own = lax.ppermute(own_near, axes, near_pairs)
        second, other_near = lax.optimization_barrier((own_near, other_near))
        other_rest = lax.ppermute(second, axes, peers)
        near_other = lax.ppermute(other_near, axes, near_pairs)
        far_other_near = lax.ppermute(other_near, axes, far_pairs)
        far_other_rest = lax.ppermute(other_rest, axes, far_pairs)
        pieces = [
            density,
            far_own,
            near_own,
            other_near,
            other_rest,
            near_other,
            far_other_near,
            far_other_rest,
        ]
        own_row = W - own_start
        far_row = jnp.where(column == 0, 0, rows + local_rows)
        near_row = jnp.where(column == 0, W + local_rows, 0)
        here = column * local_slots
        there = (1 - column) * local_slots
        firsts = [
            own_row * slots + here,
            far_row * slots + here,
            near_row * slots + here,
            (own_row + near_at) * slots + there,
            (own_row + rest_at) * slots + there,
            near_row * slots + there,
            (far_row + near_at) * slots + there,
            (far_row + rest_at) * slots + there,
        ]
        panel_rows = 2 * W + rows
    else:
        full_rows = lax.all_gather(density, "col", axis=1, tiled=True)
        pieces = [
            shifted(full_rows[local_rows - W :], 1),
            full_rows,
            shifted(full_rows[:W], -1),
        ]
        firsts = [0, W * slots, (W + local_rows) * slots]
        panel_rows = 2 * W + local_rows
    left_base = (W + own_start - panel_start) * slots
    result = products(total, left_base, firsts, lists, pieces, panel_rows, slots, rows)
    result = result.reshape(rows, slots, order, order)
    if column_count != 2:
        return lax.all_to_all(result, "col", split_axis=1, concat_axis=0, tiled=True)
    kept = lax.dynamic_slice_in_dim(result, column * local_slots, local_slots, axis=1)
    sent = lax.dynamic_slice_in_dim(result, (1 - column) * local_slots, local_slots, axis=1)
    arrived = lax.ppermute(sent, "col", [(0, 1), (1, 0)])
    return jnp.where(
        column == 0,
        jnp.concatenate([kept, arrived]),
        jnp.concatenate([arrived, kept]),
    )


def solution(mesh):
    in_specs = (P("row", "col", None, None), P("row", "col"))
    out_specs = P("row", "col", None, None)
    return jax.shard_map(
        per_device, mesh=mesh, in_specs=in_specs, out_specs=out_specs, check_vma=False
    )
```
